512 devices in a mesh: dp: 32 (over z_hi, y, core), seq: 16 (over x, z_lo).
Axes of the slice: x: 4, y: 4, z: 16 (z_hi: 4, z_lo: 4; z = z_hi * 4 + z_lo), core: 2. Of those that a mesh axis runs over, the one named last changes fastest.
Arguments:
- features: bfloat16 [32, 4096, 1024], P('dp', 'seq'), may hold values from -6 to 6
- shift_offsets: int32 [16], replicated, may hold values from -4 to 4, as said below
- conv_weight: bfloat16 [3, 1024, 1024], P(None, None, 'dp'), may hold values from -0.109375 to 0.109375
- norm_gain: float32 [1024], replicated, may hold values from 0.5 to 1.5
- query_proj: bfloat16 [32, 512, 512], P('dp', 'seq'), may hold values from -6 to 6
- key_proj: bfloat16 [32, 512, 512], P('dp', 'seq'), may hold values from -6 to 6
- value_proj: bfloat16 [32, 512, 768], P('dp', 'seq'), may hold values from -6 to 6
- head_weight: bfloat16 [1792, 512], replicated, may hold values from -0.125 to 0.125
- targets: float32 [32, 512, 512], P('dp', 'seq'), may hold values from 0 to 3
- track_mask: int32 [16, 512], replicated, may hold values from 0 to 1, as said below
- track_pairing: int32 [512], replicated, may hold values from 0 to 511, as said below
Outputs:
- features_grad: bfloat16 [32, 4096, 1024], P('dp', 'seq')
- query_grad: bfloat16 [32, 512, 512], P('dp', 'seq')
- key_grad: bfloat16 [32, 512, 512], P('dp', 'seq')
- value_grad: bfloat16 [32, 512, 768], P('dp', 'seq')
- gain_grad: float32 [1024], replicated
- mean_loss: float32 [], replicated
The draws below stay inside these ranges and needn't reach their ends.
Inputs may be any that keep to these rules, and one draw needn't show every extreme that they name: `shift_offsets`: offset in positions of each interval's 16-bp input. `track_mask`: 1 where the interval has data for the track. `track_pairing`: A pairing: applied twice it gives every track back.
All inputs are finite; a program needn't handle non-finite values.
Results may differ from the reference program's by a relative error of at most 0.028.
Values may be sent and summed in bfloat16 or wider, within the bound.
A program may use at most 64 MiB of HBM per device.

```python
import math
from functools import partial
import jax
import jax.numpy as jnp
from jax import lax

C = 1024
KW = 3
SHIFT = 4
POOL = 8
HEADS = 4
QK = 128
VD = 192
TRACKS = 512
STRANDS = 32
INTERVALS = 16
L16 = 4096
L128 = 512


def draw_shift_offsets(key, part):
    seeded = jax.random.fold_in(key, 101)
    offsets = jax.random.randint(jax.random.fold_in(seeded, 1), (INTERVALS,), -SHIFT, SHIFT + 1)
    top_slot = jax.random.randint(jax.random.fold_in(seeded, 2), (), 0, INTERVALS)
    low_slot = (top_slot + 1 + jax.random.randint(jax.random.fold_in(seeded, 3), (), 0, INTERVALS - 1)) % INTERVALS
    offsets = offsets.at[top_slot].set(SHIFT)
    offsets = offsets.at[low_slot].set(-SHIFT)
    return offsets.astype(jnp.int32)


def draw_track_mask(key, part):
    seeded = jax.random.fold_in(key, 202)
    levels = jax.random.randint(jax.random.fold_in(seeded, 1), (INTERVALS, 1), 20, 91)
    dice_rolls = jax.random.randint(jax.random.fold_in(seeded, 2), (INTERVALS, TRACKS), 0, 100)
    empty_row = jax.random.randint(jax.random.fold_in(seeded, 3), (), 0, INTERVALS)
    kept_mask = (dice_rolls < levels) & (jnp.arange(INTERVALS)[:, None] != empty_row)
    return kept_mask.astype(jnp.int32)


def draw_track_pairing(key, part):
    seeded = jax.random.fold_in(key, 303)
    shuffled = jax.random.permutation(jax.random.fold_in(seeded, 1), TRACKS).astype(jnp.int32)
    unpaired = 2 * jax.random.randint(jax.random.fold_in(seeded, 2), (), 0, TRACKS // 4 + 1)
    slot_ids = jnp.arange(TRACKS, dtype=jnp.int32)
    mate_ids = slot_ids + 1 - 2 * (slot_ids % 2)
    mate_ids = jnp.where(slot_ids < unpaired, slot_ids, mate_ids)
    pairing = jnp.zeros((TRACKS,), jnp.int32).at[shuffled].set(shuffled[mate_ids])
    return pairing.astype(jnp.int32)


def draw_entries(key):
    seeded = jax.random.fold_in(key, 404)
    full_shape = (STRANDS, L128, HEADS * QK)
    queries = jax.random.truncated_normal(jax.random.fold_in(seeded, 1), -4.0, 4.0, full_shape, jnp.float32)
    keys_out = jax.random.truncated_normal(jax.random.fold_in(seeded, 2), -4.0, 4.0, full_shape, jnp.float32)
    return (queries, keys_out)


def draw_query_proj(key, part):
    return draw_entries(key)[0].astype(jnp.bfloat16)


def draw_key_proj(key, part):
    return draw_entries(key)[1].astype(jnp.bfloat16)


def block_scale(key, extent, pieces, smallest, high):
    loudness, own = 1.0, jax.random.fold_in(key, 6)
    for position, blocks in pieces:
        heights = jnp.exp(jax.random.uniform(jax.random.fold_in(own, position), (blocks,), jnp.float32, smallest / len(pieces), high / len(pieces)))
        loudness = loudness * jnp.repeat(heights, extent[position] // blocks).reshape([-1 if axis == position else 1 for axis in range(len(extent))])
    return loudness


def normal_values(rng, extent, spread, bound, shards=(), held_as=jnp.bfloat16):
    values = jax.random.normal(rng, extent, jnp.float32) * spread
    if len(shards) > 0:
        values = block_scale(rng, extent, shards, -0.22, 0.18) * values
    return jnp.clip(values, min=-bound, max=bound).astype(held_as)


def setup_inputs(seed: int = 0) -> dict:
    key_list = jax.random.split(jax.random.key(seed), 12)
    return {
        "features": normal_values(key_list[0], (STRANDS, L16, C), 1.0, 6.0, ((0, 32), (1, 16))),
        "shift_offsets": draw_shift_offsets(jax.random.fold_in(key_list[11], 71), 0),
        "conv_weight": normal_values(key_list[2], (KW, C, C), (KW * C) ** -0.5, 0.109375, ((2, 32),)),
        "norm_gain": jnp.clip(1.0 + 0.1 * jax.random.normal(key_list[3], (C,), jnp.float32), 0.5, 1.5),
        "query_proj": draw_query_proj(jax.random.fold_in(key_list[11], 71), 0),
        "key_proj": draw_key_proj(jax.random.fold_in(key_list[11], 71), 0),
        "value_proj": normal_values(key_list[6], (STRANDS, L128, HEADS * VD), 1.0, 6.0, ((0, 32), (1, 16))),
        "head_weight": normal_values(key_list[7], (C + HEADS * VD, TRACKS), (C + HEADS * VD) ** -0.5, 0.125),
        "targets": jnp.clip(3.0 * jax.random.uniform(key_list[8], (STRANDS, L128, TRACKS), jnp.float32) ** block_scale(key_list[8], (STRANDS, L128, TRACKS), ((0, 32), (1, 16)), -0.2, 0.2), 0.0, 3.0),
        "track_mask": draw_track_mask(jax.random.fold_in(key_list[11], 71), 0),
        "track_pairing": draw_track_pairing(jax.random.fold_in(key_list[11], 71), 0),
    }


NORM_EPS = 1e-06
LOSS_SCALE = 1024.0

def to_bfloat(values):
    return lax.optimization_barrier(values.astype(jnp.bfloat16)).astype(jnp.float32)

def normalize(feats_one, shift_one):
    length = feats_one.shape[0]
    padded = jnp.pad(feats_one, ((SHIFT, SHIFT), (0, 0)))
    shifted = lax.dynamic_slice_in_dim(padded, (SHIFT - shift_one).astype(jnp.int32), length, 0)
    source = shifted.astype(jnp.float32)
    inv_rms = lax.rsqrt(lax.optimization_barrier(jnp.mean(source * source, axis=1, keepdims=True)) + NORM_EPS)
    normed = source * inv_rms
    return (source, inv_rms, normed)

def pick_tap(conv_weight, flipped, tap_idx):
    tap_pick = jnp.where(flipped, KW - 1 - tap_idx, tap_idx).astype(jnp.int32)
    return lax.dynamic_index_in_dim(conv_weight, tap_pick, 0, keepdims=False)

def attend(query_one, key_one, value_one):
    query_h = query_one.astype(jnp.float32).reshape(-1, HEADS, QK)
    key_h = key_one.astype(jnp.float32).reshape(-1, HEADS, QK)
    value_h = value_one.astype(jnp.float32).reshape(-1, HEADS, VD)
    scores = jnp.einsum('thd,lhd->htl', query_h, key_h) * (1.0 / math.sqrt(QK))
    row_max = lax.optimization_barrier(jnp.max(scores, axis=2, keepdims=True))
    exp_scores = jnp.exp(scores - row_max)
    soft_f32 = exp_scores / lax.optimization_barrier(jnp.sum(exp_scores, axis=2, keepdims=True))
    soft_b16 = to_bfloat(soft_f32)
    attended = to_bfloat(jnp.einsum('htl,lhd->thd', soft_b16, value_h).reshape(-1, HEADS * VD))
    return (query_h, key_h, value_h, soft_f32, soft_b16, attended)

def predict(conv_weight, norm_gain, head_weight, packed):
    feats_one, shift_one, flipped, query_one, key_one, value_one = packed
    length = feats_one.shape[0]
    half_taps = KW // 2
    source, inv_rms, normed = normalize(feats_one, shift_one)
    hidden = jax.nn.gelu(normed * norm_gain).astype(jnp.bfloat16)
    hidden_pad = jnp.pad(hidden, ((half_taps, half_taps), (0, 0)))
    conv_out = jnp.zeros((length, C), jnp.float32)
    for tap_idx in range(KW):
        conv_out = conv_out + jnp.dot(hidden_pad[tap_idx:tap_idx + length], pick_tap(conv_weight, flipped, tap_idx), preferred_element_type=jnp.float32)
    output = to_bfloat(source + conv_out)
    pooled = lax.optimization_barrier(jnp.mean(output.reshape(length // POOL, POOL, C), axis=1)).astype(jnp.bfloat16)
    attended = attend(query_one, key_one, value_one)[5]
    joined = jnp.concatenate([pooled, attended.astype(jnp.bfloat16)], axis=1)
    return jnp.dot(joined, head_weight, preferred_element_type=jnp.float32)

def backprop(conv_weight, norm_gain, head_weight, packed):
    feats_one, shift_one, flipped, query_one, key_one, value_one, logits, dpred_one = packed
    length = feats_one.shape[0]
    half_taps = KW // 2
    source, inv_rms, normed = normalize(feats_one, shift_one)
    gained = normed * norm_gain
    query_h, key_h, value_h, soft_f32, soft_b16, attended = attend(query_one, key_one, value_one)
    dlogit = (dpred_one * jax.nn.sigmoid(logits)).astype(jnp.bfloat16)
    djoined = lax.dot_general(dlogit, head_weight, (((1,), (1,)), ((), ())), preferred_element_type=jnp.float32)
    dpooled = djoined[:, :C]
    dattended = to_bfloat(djoined[:, C:]).reshape(-1, HEADS, VD)
    row_dots = lax.optimization_barrier(jnp.sum(dattended * attended.reshape(-1, HEADS, VD), axis=2))
    dprobs = jnp.einsum('thd,lhd->htl', dattended, value_h)
    dscore = to_bfloat(soft_f32 * (dprobs - row_dots.T[:, :, None]))
    inv_sqrt = 1.0 / math.sqrt(QK)
    query_grad = (jnp.einsum('htl,lhd->thd', dscore, key_h) * inv_sqrt).reshape(-1, HEADS * QK).astype(jnp.bfloat16)
    key_grad = (jnp.einsum('htl,thd->lhd', dscore, query_h) * inv_sqrt).reshape(-1, HEADS * QK).astype(jnp.bfloat16)
    value_grad = jnp.einsum('htl,thd->lhd', soft_b16, dattended).reshape(-1, HEADS * VD).astype(jnp.bfloat16)
    dgrad_f32 = jnp.repeat(dpooled / POOL, POOL, axis=0)
    dgrad_pad = jnp.pad(dgrad_f32.astype(jnp.bfloat16), ((half_taps, half_taps), (0, 0)))
    dhidden = jnp.zeros((length, C), jnp.float32)
    for tap_idx in range(KW):
        tap_start = KW - 1 - tap_idx
        dhidden = dhidden + lax.dot_general(dgrad_pad[tap_start:tap_start + length], pick_tap(conv_weight, flipped, tap_idx), (((1,), (1,)), ((), ())), preferred_element_type=jnp.float32)
    unused, gelu_back = jax.vjp(jax.nn.gelu, gained)
    dgained = gelu_back(dhidden)[0]
    gain_part = lax.optimization_barrier(jnp.sum(dgained * normed, axis=0))
    dnormed = dgained * norm_gain
    dsource = inv_rms * (dnormed - normed * lax.optimization_barrier(jnp.mean(dnormed * normed, axis=1, keepdims=True))) + dgrad_f32
    dpadded = jnp.pad(dsource.astype(jnp.bfloat16), ((SHIFT, SHIFT), (0, 0)))
    features_grad = lax.dynamic_slice_in_dim(dpadded, (SHIFT + shift_one).astype(jnp.int32), length, 0)
    return (features_grad, query_grad, key_grad, value_grad, gain_part)

def reference(features, shift_offsets, conv_weight, norm_gain, query_proj, key_proj, value_proj, head_weight, targets, track_mask, track_pairing):
    signed = jnp.concatenate([shift_offsets, -shift_offsets]).astype(jnp.int32)
    flip_rows = jnp.arange(STRANDS) >= INTERVALS
    logits = lax.map(partial(predict, conv_weight, norm_gain, head_weight), (features, signed, flip_rows, query_proj, key_proj, value_proj))
    predicted = jax.nn.softplus(logits)
    mask_rows = jnp.concatenate([track_mask, track_mask], axis=0).astype(jnp.float32)
    counted = jnp.maximum(lax.optimization_barrier(jnp.sum(mask_rows, axis=1)), 1.0)[:, None, None]
    partner = jnp.roll(predicted, INTERVALS, axis=0)
    misfit = 0.5 * (predicted + jnp.take(partner, track_pairing, axis=2)) - targets
    weighted = mask_rows[:, None, :] * misfit
    mean_loss = jnp.sum(weighted * misfit / counted) / (STRANDS * L128)
    slopes = 2.0 * LOSS_SCALE * weighted / counted
    dpredicted = 0.5 * (slopes + jnp.take(jnp.roll(slopes, INTERVALS, axis=0), track_pairing, axis=2))
    gradients = lax.map(partial(backprop, conv_weight, norm_gain, head_weight), (features, signed, flip_rows, query_proj, key_proj, value_proj, logits, dpredicted))
    features_grad, query_grad, key_grad, value_grad, gain_parts = gradients
    return (features_grad, query_grad, key_grad, value_grad, lax.optimization_barrier(jnp.sum(gain_parts, axis=0)), mean_loss)
```

```python
import math

import jax
import jax.numpy as jnp
from jax import lax
from jax.experimental import pallas as pl
from jax.experimental.pallas import tpu as pltpu
from jax.sharding import PartitionSpec as P

KW = 3
SHIFT = 4
POOL = 8
HEADS = 4
QK = 128
VD = 192
C = 1024
TRACKS = 512
ROWS = 256
TOK = 32
L16 = 4096
PAIRS = 16
RIM = 16
VP = 256
ROW = 1152
NORM_EPS = 1e-06
LOSS_SCALE = 1024.0
ROOT = math.sqrt(2.0 / math.pi)
CUBIC = 0.044715
COPIES = 136
f32 = jnp.float32
bf16 = jnp.bfloat16

NT = (((1,), (1,)), ((), ()))
NN = (((1,), (0,)), ((), ()))
TN = (((0,), (0,)), ((), ()))


def dot(a, b, dims):
    return lax.dot_general(a, b, dims, preferred_element_type=f32)


def iota(shape, axis):
    return lax.broadcasted_iota(jnp.int32, shape, axis)


class Copies:
    def __init__(self, send, recv):
        self.send, self.recv, self.used, self.sent = send, recv, 0, []

    def start(self, src, dst, device):
        n = self.used
        self.used += 1
        copy = pltpu.make_async_remote_copy(
            src_ref=src,
            dst_ref=dst,
            send_sem=self.send.at[n],
            recv_sem=self.recv.at[n],
            device_id=device,
            device_id_type=pl.DeviceIdType.MESH,
        )
        copy.start()
        self.sent.append(copy)
        return n

    def arrived(self, n, dst):
        pltpu.make_async_remote_copy(
            src_ref=dst,
            dst_ref=dst,
            send_sem=self.send.at[n],
            recv_sem=self.recv.at[n],
            device_id=self.someone,
            device_id_type=pl.DeviceIdType.MESH,
        ).wait_recv()

    def finish(self):
        for copy in self.sent:
            copy.wait_send()


class Gather:
    def __init__(self, copies, device, unit):
        self.copies, self.device, self.unit = copies, device, unit

    def begin(self):
        mine = self.unit(0, None)
        self.right = self.copies.start(mine, mine, self.device(1))
        self.left = self.copies.start(mine, mine, self.device(3))

    def relay(self):
        self.copies.arrived(self.right, self.unit(3, None))
        part = self.unit(3, 0)
        self.far_right = self.copies.start(part, part, self.device(1))
        self.copies.arrived(self.left, self.unit(1, None))
        part = self.unit(1, 1)
        self.far_left = self.copies.start(part, part, self.device(3))

    def end(self):
        self.copies.arrived(self.far_right, self.unit(2, 0))
        self.copies.arrived(self.far_left, self.unit(2, 1))


def step_kernel(
    feats_in,
    offsets_in,
    wt_in,
    gain_in,
    query_in,
    key_in,
    value_in,
    head_in,
    targets_in,
    mask_in,
    pairing_in,
    dfeats,
    dquery,
    dkey,
    dvalue,
    dgain,
    loss_out,
    offsets,
    gain,
    value,
    targets,
    track_mask,
    pairing,
    wf,
    fext,
    hext,
    nbuf,
    dbuf,
    rbuf,
    head,
    qkv,
    kva,
    att_s,
    att_r,
    probs,
    probs_b,
    taps,
    pooled_u,
    pooled,
    pred_s,
    pred_r,
    tgt_r,
    pick,
    tgt_p,
    datt_s,
    datt_r,
    dq_s,
    dq_r,
    kvp_s,
    kvp_r,
    kvg_s,
    kvg_r,
    dyt,
    zhi,
    zlo,
    dyhl,
    dhb,
    dyb,
    gacc,
    ar_c,
    ar_y,
    ar_x,
    ar_l,
    ar_h,
    send_sem,
    recv_sem,
    own_sem,
):
    dp = lax.axis_index("dp")
    s = lax.axis_index("seq")
    zh, y, c = lax.div(dp, 8), lax.rem(lax.div(dp, 2), 4), lax.rem(dp, 2)
    x, zl = lax.div(s, 4), lax.rem(s, 4)

    def turn(a, o):
        return lax.rem(a + o, 4)

    def at_y(o):
        return {"dp": zh * 8 + turn(y, o) * 2 + c, "seq": s}

    def at_zh(o):
        return {"dp": turn(zh, o) * 8 + y * 2 + c, "seq": s}

    def at_x(o):
        return {"dp": dp, "seq": turn(x, o) * 4 + zl}

    def at_zl(o):
        return {"dp": dp, "seq": x * 4 + turn(zl, o)}

    other = {"dp": zh * 8 + y * 2 + (1 - c), "seq": s}
    after = {"dp": dp, "seq": lax.rem(s + 1, 16)}
    before = {"dp": dp, "seq": lax.rem(s + 15, 16)}

    barrier = pltpu.get_barrier_semaphore()
    peers = [f(o) for f in (at_y, at_zh, at_x, at_zl) for o in (1, 2, 3)]
    peers += [other, after, before]
    for peer in peers:
        pl.semaphore_signal(
            barrier, inc=1, device_id=peer, device_id_type=pl.DeviceIdType.MESH
        )
    copies = Copies(send_sem, recv_sem)
    copies.someone = other

    pulls = []

    def pull(src, dst):
        pulls.append(pltpu.make_async_copy(src, dst, own_sem.at[len(pulls)]))
        pulls[-1].start()
        return pulls[-1]

    wt_pull = pull(wt_in, wf.at[:, zh, y, c])
    qkv_pulls = [pull(value_in, value)]
    for h in range(HEADS):
        cols = pl.ds(h * QK, QK)
        qkv_pulls.append(pull(query_in.at[:, cols], qkv.at[h, :, pl.ds(0, QK)]))
        qkv_pulls.append(pull(key_in.at[:, cols], qkv.at[h, :, pl.ds(QK, QK)]))
    feats_pulls = [pull(gain_in, gain), pull(feats_in, fext.at[pl.ds(RIM, ROWS)])]
    rest_pulls = [
        pull(targets_in, targets),
        pull(offsets_in, offsets),
        pull(mask_in, track_mask),
        pull(pairing_in, pairing),
    ]
    rows = C + HEADS * VD
    head_copy = pull(head_in, head.at[pl.ds(0, rows)])
    head[rows:, :] = jnp.zeros((VP - VD, TRACKS), bf16)

    for one in qkv_pulls:
        one.wait()
    lane = iota((TOK, VP), 1)
    vals = value[...].astype(f32)
    for h in range(HEADS):
        start = h * VD
        if h % 2 == 0:
            cut = vals[:, start : start + VP]
        else:
            cut = pltpu.roll(vals[:, start - 64 : start + VD], VP - 64, 1)
        qkv[h, :, 2 * QK :] = jnp.where(lane < VD, cut, 0.0).astype(bf16)
    kva[zl, x] = qkv[x]
    for one in feats_pulls:
        one.wait()

    def pointwise(row):
        f = fext[pl.ds(row, 16), :].astype(f32)
        r = lax.rsqrt(jnp.mean(f * f, axis=1, keepdims=True) + NORM_EPS)
        n = f * r
        g = n * gain[...]
        sq = g * g
        t = jnp.tanh(ROOT * (g + CUBIC * (sq * g)))
        hext[pl.ds(row, 16), :] = (0.5 * g * (1.0 + t)).astype(bf16)
        slope = 0.5 * (1.0 + t) + (0.5 * ROOT) * g * (1.0 - t * t) * (
            1.0 + (3.0 * CUBIC) * sq
        )
        return n, slope, r

    @pl.loop(0, ROWS // 16)
    def _(i):
        row = pl.multiple_of(i * 16, 16)
        n, slope, r = pointwise(pl.multiple_of(row + RIM, 16))
        nbuf[pl.ds(row, 16), :] = n
        dbuf[pl.ds(row, 16), :] = slope
        rbuf[pl.ds(row, 16), :] = jnp.broadcast_to(r, (16, 128))

    for one in rest_pulls:
        one.wait()
    wt_pull.wait()
    pl.semaphore_wait(barrier, len(peers))

    lo = copies.start(fext.at[pl.ds(ROWS, RIM)], fext.at[pl.ds(0, RIM)], after)
    hi = copies.start(fext.at[pl.ds(RIM, RIM)], fext.at[pl.ds(RIM + ROWS, RIM)], before)
    qkv_in = [
        copies.start(qkv.at[turn(x, o)], kva.at[zl, x], at_x(o)) for o in (1, 2, 3)
    ]

    def columns(o, half):
        if half is None:
            return pl.ds(pl.multiple_of(turn(x, o) * 256, 128), 256)
        return pl.ds(pl.multiple_of(turn(x, o) * 256 + 128 * half, 128), 128)

    def unit_xy(r):
        return lambda o, half: wf.at[:, turn(zh, r), turn(y, o), c, 0, :, columns(0, half)]

    def unit_yx(r):
        return lambda o, half: wf.at[:, turn(zh, r), y, c, :, :, columns(o, half)]

    def unit_xx(r):
        return lambda o, half: wf.at[:, :, turn(y, r), c, 0, :, columns(o, half)]

    def unit_yy(r):
        def unit(o, half):
            cols = pl.ds(0, C) if half is None else pl.ds(half * 512, 512)
            return wf.at[:, turn(zh, r), turn(y, o), c, 1, :, cols]

        return unit

    g_xy = [Gather(copies, at_y, unit_xy(r)) for r in range(4)]
    g_yx = [Gather(copies, at_x, unit_yx(r)) for r in range(4)]
    g_xx = [Gather(copies, at_x, unit_xx(r)) for r in range(4)]
    g_yy = [Gather(copies, at_y, unit_yy(r)) for r in range(4)]

    def piece(r):
        return wf.at[:, turn(zh, r), y, c, :, :, columns(0, None)]

    g_xy[0].begin()
    g_yy[0].begin()
    z_in = {r: copies.start(piece(0), piece(0), at_zh(4 - r)) for r in (1, 3, 2)}
    tgt_in = copies.start(targets, tgt_r, at_zh(2))

    flip = dp >= PAIRS
    interval = lax.rem(dp, PAIRS)
    sign = jnp.where(flip, -1, 1)
    mine = iota((1, PAIRS), 1) == interval
    chosen = jnp.sum(jnp.where(mine, offsets[...].astype(f32), 0.0), axis=1, keepdims=True)
    off = chosen.astype(jnp.int32) * sign

    copies.arrived(lo, fext.at[pl.ds(0, RIM)])
    copies.arrived(hi, fext.at[pl.ds(RIM + ROWS, RIM)])
    pointwise(0)
    pointwise(RIM + ROWS)
    EXT = ROWS + 2 * RIM

    def mean_matrix(count, shift_of):
        row, col = iota((count, EXT), 0), iota((count, EXT), 1)
        tok = lax.rem(row, TOK)
        at = col - RIM
        rel = at + off - shift_of(row) - POOL * tok
        where_p = s * ROWS + at + off
        where_q = s * ROWS + at
        fine = (rel >= 0) & (rel < POOL) & (where_p >= 0) & (where_p < L16)
        fine = fine & (where_q >= 0) & (where_q < L16)
        return jnp.where(fine, 1.0 / POOL, 0.0).astype(bf16)

    mix = mean_matrix(KW * TOK, lambda row: (lax.div(row, TOK) - 1) * sign)
    taps[...] = dot(mix, hext[...], NN).astype(bf16)
    mix = mean_matrix(TOK, lambda row: 0 * row)
    pooled_u[...] = dot(mix, fext[...], NN)

    for o, n in zip((1, 2, 3), qkv_in):
        copies.arrived(n, kva.at[zl, turn(x, 4 - o)])
    kv_cols = pl.ds(QK, 3 * QK)
    kv_in = [
        copies.start(kva.at[zl, :, :, kv_cols], kva.at[zl, :, :, kv_cols], at_zl(o))
        for o in (1, 2, 3)
    ]

    g_xy[0].relay()
    copies.arrived(z_in[1], piece(1))
    g_yx[1].begin()
    g_xy[1].begin()
    copies.arrived(z_in[3], piece(3))
    g_yx[3].begin()
    g_xy[3].begin()
    g_yy[0].relay()
    g_yx[1].relay()
    g_yx[3].relay()
    copies.arrived(z_in[2], piece(2))
    g_yx[2].begin()
    g_xy[2].begin()
    g_xy[1].relay()
    g_xy[3].relay()
    g_yx[1].end()
    g_yy[1].begin()
    g_yx[3].end()
    g_yy[3].begin()
    g_yx[2].relay()
    g_xy[2].relay()
    g_xx[1].begin()
    g_xx[3].begin()
    g_yx[2].end()
    g_yy[2].begin()
    for r in (0, 1, 3, 2):
        g_xy[r].end()
    g_xx[2].begin()
    g_yy[1].relay()

    for o, n in zip((1, 2, 3), kv_in):
        copies.arrived(n, kva.at[turn(zl, 4 - o), :, :, kv_cols])
    inv_sqrt = 1.0 / math.sqrt(QK)
    qh = kva[zl, :, :, 0:QK].reshape(4 * TOK, QK)
    kh = kva[:, :, :, QK : 2 * QK].reshape(16 * TOK, QK)
    vh = kva[:, :, :, 2 * QK :].reshape(16 * TOK, VP)
    scores = dot(qh, kh, NT) * inv_sqrt
    e = jnp.exp(scores - jnp.max(scores, axis=1, keepdims=True))
    p = e / jnp.sum(e, axis=1, keepdims=True)
    probs[...] = p
    probs_b[...] = p.astype(bf16)
    att_s[...] = dot(probs_b[...], vh, NN).astype(bf16).reshape(4, TOK, VP)
    att_r[x] = att_s[x]
    att_in = [
        copies.start(att_s.at[turn(x, o)], att_r.at[x], at_x(o)) for o in (1, 2, 3)
    ]

    g_xx[1].relay()
    g_yy[3].relay()
    g_xx[3].relay()
    g_yy[2].relay()
    g_xx[2].relay()

    pick[...] = jnp.where(
        iota((TRACKS, TRACKS), 0) == pairing[...], 1.0, 0.0
    ).astype(bf16)
    copies.arrived(tgt_in, tgt_r)
    theirs = tgt_r[...]
    coarse = theirs.astype(bf16)
    fine = (theirs - coarse.astype(f32)).astype(bf16)
    tgt_p[...] = dot(coarse, pick[...], NN) + dot(fine, pick[...], NN)
    mrow = track_mask[pl.ds(interval, 1), :].astype(f32)
    count = jnp.maximum(jnp.sum(mrow, axis=1, keepdims=True), 1.0)
    mpair = dot(jnp.broadcast_to(mrow, (16, TRACKS)).astype(bf16), pick[...], NN)[0:1, :]

    pair_in = []

    def share_x(r):
        part = wf.at[:, :, turn(y, r), c, 0]
        pair_in.append((copies.start(part, part, other), wf.at[:, :, turn(y, r), 1 - c, 0]))

    def share_y(r):
        part = wf.at[:, turn(zh, r), :, c, 1]
        pair_in.append((copies.start(part, part, other), wf.at[:, turn(zh, r), :, 1 - c, 1]))

    g_yy[0].end()
    share_y(0)
    share_x(0)
    g_yy[1].end()
    share_y(1)
    g_xx[1].end()
    share_x(1)
    g_yy[3].end()
    share_y(3)
    g_xx[3].end()
    share_x(3)
    g_yy[2].end()
    share_y(2)
    g_xx[2].end()
    share_x(2)
    for o, n in zip((1, 2, 3), att_in):
        copies.arrived(n, att_r.at[turn(x, 4 - o)])
    head_copy.wait()
    for n, part in pair_in:
        copies.arrived(n, part)

    @pl.loop(0, 4)
    def _(b):
        cols = pl.ds(pl.multiple_of(b * 256, 256), 256)
        acc = pooled_u[:, cols]
        for t in range(KW):
            w = wf[t, b].reshape(256, C)
            acc = acc + dot(taps[t * TOK : (t + 1) * TOK, :], w, NT)
        pooled[:, cols] = acc.astype(bf16)

    logits = dot(pooled[...], head[0:C, :], NN)
    for h in range(HEADS):
        logits = logits + dot(att_r[h], head[C + h * VD : C + h * VD + VP, :], NN)
    pred = jnp.maximum(logits, 0.0) + jnp.log1p(jnp.exp(-jnp.abs(logits)))
    pred_s[...] = pred.astype(bf16)
    pred_in = copies.start(pred_s, pred_r, at_zh(2))
    gate = jax.nn.sigmoid(logits)
    copies.arrived(pred_in, pred_r)
    both = 0.5 * (pred + dot(pred_r[...], pick[...], NN))
    misfit = both - targets[...]
    weighted = mrow * misfit
    loss = jnp.sum(jnp.sum(weighted * misfit, axis=1, keepdims=True), axis=0, keepdims=True)
    loss = loss / count / (2.0 * PAIRS * TOK * 16)
    dpred = (LOSS_SCALE / count) * (weighted + mpair * (both - tgt_p[...]))
    dlogit = (dpred * gate).astype(bf16)

    for h in range(HEADS):
        part = dot(dlogit, head[C + h * VD : C + h * VD + VP, :], NT)
        datt_s[h] = jnp.where(lane < VD, part, 0.0).astype(bf16)
    datt_r[x] = datt_s[x]
    datt_in = [
        copies.start(datt_s.at[turn(x, o)], datt_r.at[x], at_x(o)) for o in (1, 2, 3)
    ]
    dyt[8 : 8 + TOK, :] = dot(dlogit, head[0:C, :], NT) * (1.0 / POOL)
    dyt[48:, :] = jnp.zeros((16, C), f32)
    tok_lo = copies.start(dyt.at[pl.ds(TOK, 8)], dyt.at[pl.ds(0, 8)], after)
    tok_hi = copies.start(dyt.at[pl.ds(8, 8)], dyt.at[pl.ds(8 + TOK, 8)], before)

    for o, n in zip((1, 2, 3), datt_in):
        copies.arrived(n, datt_r.at[turn(x, 4 - o)])
    dout = datt_r[...].reshape(4 * TOK, VP)
    att = att_s[...].reshape(4 * TOK, VP)
    delta = jnp.sum(dout.astype(f32) * att.astype(f32), axis=1, keepdims=True)
    vh = kva[:, :, :, 2 * QK :].reshape(16 * TOK, VP)
    ds = (probs[...] * (dot(dout, vh, NT) - delta)).astype(bf16)
    qh = kva[zl, :, :, 0:QK].reshape(4 * TOK, QK)
    kvp_s[:, :, :, 0:QK] = dot(ds, qh, TN).astype(bf16).reshape(4, 4, TOK, QK)
    kvp_s[:, :, :, QK:] = dot(probs_b[...], dout, TN).astype(bf16).reshape(4, 4, TOK, VP)
    kvp_in = [
        copies.start(kvp_s.at[turn(zl, o)], kvp_r.at[zl], at_zl(o)) for o in (1, 2, 3)
    ]
    kh = kva[:, :, :, QK : 2 * QK].reshape(16 * TOK, QK)
    dq_s[...] = (dot(ds, kh, NN) * inv_sqrt).astype(bf16).reshape(4, TOK, QK)
    dq_r[x] = dq_s[x]
    dq_in = [copies.start(dq_s.at[turn(x, o)], dq_r.at[x], at_x(o)) for o in (1, 2, 3)]

    copies.arrived(tok_lo, dyt.at[pl.ds(0, 8)])
    copies.arrived(tok_hi, dyt.at[pl.ds(8 + TOK, 8)])
    dy = dyt[...]
    dyc = dy.astype(bf16)
    dyhl[0:64, :] = dyc
    dyhl[64:, :] = (dy - dyc.astype(f32)).astype(bf16)

    @pl.loop(0, 4)
    def _(b):
        cols = pl.ds(pl.multiple_of(b * 256, 256), 256)
        for t in range(KW):
            acc = jnp.zeros((64, 256), f32)
            for z in range(4):
                w = wf[t, z, :, :, :, :, cols].reshape(256, 256)
                acc = acc + dot(dyhl[0:64, z * 256 : (z + 1) * 256], w, NN)
            top = acc.astype(bf16)
            zhi[t * 64 : (t + 1) * 64, cols] = top
            zlo[t * 64 : (t + 1) * 64, cols] = (acc - top.astype(f32)).astype(bf16)

    def spread(width, tap_of):
        row, col = iota((ROWS, width), 0), iota((ROWS, width), 1)
        reach = row + off - tap_of(col)
        at = s * ROWS + row + off
        seen = s * ROWS + reach
        fine = (lax.shift_right_arithmetic(reach + 64, 3) == lax.rem(col, 64)) & (at >= 0)
        fine = fine & (at < L16) & (seen >= 0) & (seen < L16)
        return jnp.where(fine, 1.0, 0.0).astype(bf16)

    three = spread(192, lambda col: (lax.div(col, 64) - 1) * sign)
    two = spread(128, lambda col: 0 * col)

    @pl.loop(0, 4)
    def _(b):
        cols = pl.ds(pl.multiple_of(b * 256, 256), 256)
        dhb[:, cols] = dot(three, zhi[:, cols], NN) + dot(three, zlo[:, cols], NN)
        dyb[:, cols] = dot(two, dyhl[:, cols], NN)

    gacc[...] = jnp.zeros((8, C), f32)

    @pl.loop(0, ROWS // 16)
    def _(i):
        at = pl.ds(pl.multiple_of(i * 16, 16), 16)
        n = nbuf[at, :]
        dg = dhb[at, :] * dbuf[at, :]
        each = dg * n
        gacc[...] += each[0:8, :] + each[8:16, :]
        mid = jnp.mean(each * gain[...], axis=1, keepdims=True)
        r = rbuf[at, :][:, 0:1]
        dfeats[at, :] = (r * (dg * gain[...] - n * mid) + dyb[at, :]).astype(bf16)

    def all_sum(buf, mine, total, device, offs):
        buf[mine] = total
        ins = [copies.start(buf.at[mine], buf.at[mine], device(o)) for o in offs]
        return ins

    def sum_of(buf, mine, ins, offs):
        for o, n in zip(offs, ins):
            copies.arrived(n, buf.at[turn(mine, 4 - o)])
        return (buf[0] + buf[1]) + (buf[2] + buf[3])

    own = jnp.concatenate(
        [jnp.sum(gacc[...], axis=0, keepdims=True), jnp.broadcast_to(loss, (1, 128))], axis=1
    )
    ar_c[c] = own
    n = copies.start(ar_c.at[c], ar_c.at[c], other)
    copies.arrived(n, ar_c.at[1 - c])
    offs = (1, 2, 3)
    ins = all_sum(ar_h, zh, ar_c[0] + ar_c[1], at_zh, offs)

    for o, n in zip(offs, kvp_in):
        copies.arrived(n, kvp_r.at[turn(zl, 4 - o)])
    total = kvp_s[zl].astype(f32)
    for o in offs:
        total = total + kvp_r[turn(zl, o)].astype(f32)
    kvg_s[:, :, 0:QK] = (total[:, :, 0:QK] * inv_sqrt).astype(bf16)
    kvg_s[:, :, QK:] = total[:, :, QK:].astype(bf16)
    kvg_r[x] = kvg_s[x]
    kvg_in = [
        copies.start(kvg_s.at[turn(x, o)], kvg_r.at[x], at_x(o)) for o in (1, 2, 3)
    ]
    for o, n in zip(offs, dq_in):
        copies.arrived(n, dq_r.at[turn(x, 4 - o)])
    for h in range(HEADS):
        dquery[:, h * QK : (h + 1) * QK] = dq_r[h]
    for o, n in zip(offs, kvg_in):
        copies.arrived(n, kvg_r.at[turn(x, 4 - o)])
    for h in range(HEADS):
        dkey[:, h * QK : (h + 1) * QK] = kvg_r[h, :, 0:QK]
    for h in (0, 2):
        even = kvg_r[h, :, QK:].astype(f32)
        odd = pltpu.roll(kvg_r[h + 1, :, QK:].astype(f32), VD, 1)
        start = h * VD
        dvalue[:, start : start + VP] = jnp.where(lane < VD, even, odd).astype(bf16)
        dvalue[:, start + VP : start + VP + 128] = odd[:, 0:128].astype(bf16)

    total = sum_of(ar_h, zh, ins, offs)
    for buf, mine, device in ((ar_l, zl, at_zl), (ar_x, x, at_x), (ar_y, y, at_y)):
        ins = all_sum(buf, mine, total, device, offs)
        total = sum_of(buf, mine, ins, offs)
    dgain[...] = total[:, 0:C]
    loss_out[...] = total[:, C:]
    copies.finish()


def store_kernel(*refs):
    sems = refs[12]
    puts = [pltpu.make_async_copy(refs[i], refs[6 + i], sems.at[i]) for i in range(6)]
    for put in puts:
        put.start()
    for put in puts:
        put.wait()


def body(
    features,
    shift_offsets,
    conv_weight,
    norm_gain,
    query_proj,
    key_proj,
    value_proj,
    head_weight,
    targets,
    track_mask,
    track_pairing,
):
    wt = jnp.swapaxes(conv_weight, 1, 2).reshape(KW, 2, 16, C)
    vmem = pl.BlockSpec(memory_space=pltpu.VMEM)
    hbm = pl.BlockSpec(memory_space=pltpu.HBM)
    V = pltpu.VMEM
    scratch = [
        V((1, PAIRS), jnp.int32),
        V((1, C), f32),
        V((TOK, HEADS * VD), bf16),
        V((TOK, TRACKS), f32),
        V((PAIRS, TRACKS), jnp.int32),
        V((1, TRACKS), jnp.int32),
        V((KW, 4, 4, 2, 2, 16, C), bf16),
        V((ROWS + 2 * RIM, C), bf16),
        V((ROWS + 2 * RIM, C), bf16),
        V((ROWS, C), f32),
        V((ROWS, C), f32),
        V((ROWS, 128), f32),
        V((C + HEADS * VD + VP - VD, TRACKS), bf16),
        V((4, TOK, 512), bf16),
        V((4, 4, TOK, 512), bf16),
        V((4, TOK, VP), bf16),
        V((4, TOK, VP), bf16),
        V((4 * TOK, 16 * TOK), f32),
        V((4 * TOK, 16 * TOK), bf16),
        V((KW * TOK, C), bf16),
        V((TOK, C), f32),
        V((TOK, C), bf16),
        V((TOK, TRACKS), bf16),
        V((TOK, TRACKS), bf16),
        V((TOK, TRACKS), f32),
        V((TRACKS, TRACKS), bf16),
        V((TOK, TRACKS), f32),
        V((4, TOK, VP), bf16),
        V((4, TOK, VP), bf16),
        V((4, TOK, QK), bf16),
        V((4, TOK, QK), bf16),
        V((4, 4, TOK, 384), bf16),
        V((4, 4, TOK, 384), bf16),
        V((4, TOK, 384), bf16),
        V((4, TOK, 384), bf16),
        V((64, C), f32),
        V((192, C), bf16),
        V((192, C), bf16),
        V((128, C), bf16),
        V((ROWS, C), f32),
        V((ROWS, C), f32),
        V((8, C), f32),
        V((2, 1, ROW), f32),
        V((4, 1, ROW), f32),
        V((4, 1, ROW), f32),
        V((4, 1, ROW), f32),
        V((4, 1, ROW), f32),
        pltpu.SemaphoreType.DMA((COPIES,)),
        pltpu.SemaphoreType.DMA((COPIES,)),
        pltpu.SemaphoreType.DMA((20,)),
    ]
    out = jax.ShapeDtypeStruct
    outs = pl.pallas_call(
        step_kernel,
        name="strand_step",
        out_shape=(
            out((ROWS, C), bf16),
            out((TOK, HEADS * QK), bf16),
            out((TOK, HEADS * QK), bf16),
            out((TOK, HEADS * VD), bf16),
            out((1, C), f32),
            out((1, 128), f32),
        ),
        in_specs=[hbm] * 11,
        out_specs=(vmem,) * 6,
        scratch_shapes=scratch,
        compiler_params=pltpu.CompilerParams(
            collective_id=0, has_side_effects=True, vmem_limit_bytes=48 << 20
        ),
    )(
        *(
            pltpu.with_memory_space_constraint(a, pltpu.HBM)
            for a in (
                features[0],
                shift_offsets.reshape(1, PAIRS),
                wt,
                norm_gain.reshape(1, C),
                query_proj[0],
                key_proj[0],
                value_proj[0],
                head_weight,
                targets[0],
                track_mask,
                track_pairing.reshape(1, TRACKS),
            )
        )
    )
    outs = pl.pallas_call(
        store_kernel,
        name="store",
        out_shape=tuple(out(o.shape, o.dtype) for o in outs),
        in_specs=[vmem] * 6,
        out_specs=(hbm,) * 6,
        scratch_shapes=[pltpu.SemaphoreType.DMA((6,))],
        compiler_params=pltpu.CompilerParams(vmem_limit_bytes=4 << 20),
    )(*outs)
    features_grad, query_grad, key_grad, value_grad, gain_grad, loss = outs
    return (
        features_grad[None],
        query_grad[None],
        key_grad[None],
        value_grad[None],
        gain_grad.reshape(C),
        loss[0, 0],
    )


def solution(mesh):
    placed = (
        P("dp", "seq", None),
        P(),
        P(None, None, "dp"),
        P(),
        P("dp", "seq", None),
        P("dp", "seq", None),
        P("dp", "seq", None),
        P(),
        P("dp", "seq", None),
        P(),
        P(),
    )
    return jax.shard_map(
        body,
        mesh=mesh,
        in_specs=placed,
        out_specs=(
            P("dp", "seq", None),
            P("dp", "seq", None),
            P("dp", "seq", None),
            P("dp", "seq", None),
            P(),
            P(),
        ),
        check_vma=False,
    )
```

```python
import math

import jax
import jax.numpy as jnp
from jax import lax
from jax.experimental import pallas as pl
from jax.experimental.pallas import tpu as pltpu
from jax.sharding import PartitionSpec as P

KW = 3
SHIFT = 4
POOL = 8
HEADS = 4
QK = 128
VD = 192
C = 1024
TRACKS = 512
ROWS = 256
TOK = 32
L16 = 4096
PAIRS = 16
RIM = 16
VP = 256
ROW = 1152
NORM_EPS = 1e-06
LOSS_SCALE = 1024.0
ROOT = math.sqrt(2.0 / math.pi)
CUBIC = 0.044715
COPIES = 136
f32 = jnp.float32
bf16 = jnp.bfloat16

NT = (((1,), (1,)), ((), ()))
NN = (((1,), (0,)), ((), ()))
TN = (((0,), (0,)), ((), ()))


def dot(a, b, dims):
    return lax.dot_general(a, b, dims, preferred_element_type=f32)


def iota(shape, axis):
    return lax.broadcasted_iota(jnp.int32, shape, axis)


class Copies:
    def __init__(self, send, recv):
        self.send, self.recv, self.used, self.sent = send, recv, 0, []

    def start(self, src, dst, device):
        n = self.used
        self.used += 1
        copy = pltpu.make_async_remote_copy(
            src_ref=src,
            dst_ref=dst,
            send_sem=self.send.at[n],
            recv_sem=self.recv.at[n],
            device_id=device,
            device_id_type=pl.DeviceIdType.MESH,
        )
        copy.start()
        self.sent.append(copy)
        return n

    def arrived(self, n, dst):
        pltpu.make_async_remote_copy(
            src_ref=dst,
            dst_ref=dst,
            send_sem=self.send.at[n],
            recv_sem=self.recv.at[n],
            device_id=self.someone,
            device_id_type=pl.DeviceIdType.MESH,
        ).wait_recv()

    def finish(self):
        for copy in self.sent:
            copy.wait_send()


class Gather:
    def __init__(self, copies, device, unit):
        self.copies, self.device, self.unit = copies, device, unit

    def begin(self):
        mine = self.unit(0, None)
        self.right = self.copies.start(mine, mine, self.device(1))
        self.left = self.copies.start(mine, mine, self.device(3))

    def relay_from_left(self):
        self.copies.arrived(self.right, self.unit(3, None))
        part = self.unit(3, 0)
        self.far_right = self.copies.start(part, part, self.device(1))

    def relay_from_right(self):
        self.copies.arrived(self.left, self.unit(1, None))
        part = self.unit(1, 1)
        self.far_left = self.copies.start(part, part, self.device(3))

    def relay(self):
        self.relay_from_left()
        self.relay_from_right()

    def end(self):
        self.copies.arrived(self.far_right, self.unit(2, 0))
        self.copies.arrived(self.far_left, self.unit(2, 1))


class Direct(Gather):
    def begin(self):
        mine = self.unit(0, None)
        self.ins = [(o, self.copies.start(mine, mine, self.device(o))) for o in (1, 3, 2)]

    def end(self):
        for o, n in self.ins:
            self.copies.arrived(n, self.unit(4 - o, None))


def step_kernel(
    feats_in,
    offsets_in,
    wt_in,
    gain_in,
    query_in,
    key_in,
    value_in,
    head_in,
    targets_in,
    mask_in,
    pairing_in,
    dfeats,
    dquery,
    dkey,
    dvalue,
    dgain,
    loss_out,
    offsets,
    gain,
    value,
    targets,
    track_mask,
    pairing,
    wf,
    fext,
    hext,
    dnh,
    dnl,
    nbuf,
    dbuf,
    rbuf,
    head,
    headp,
    qkv,
    kva,
    att_s,
    att_r,
    probs,
    probs_b,
    taps,
    weigh,
    cv_s,
    cv_r,
    dyp_s,
    dyp_r,
    zp_s,
    zp_r,
    pre,
    pred_s,
    pred_r,
    tgt_s,
    tgt_r,
    pick,
    tgt_p,
    three,
    one,
    datt_s,
    datt_r,
    dq_s,
    dq_r,
    kvp_s,
    kvp_r,
    kvg_s,
    kvg_r,
    dyt,
    zall,
    rim_s,
    rim_r,
    dhb,
    dyb,
    gacc,
    ar_c,
    ar_p,
    ar_l,
    ar_h,
    send_sem,
    recv_sem,
    own_sem,
):
    dp = lax.axis_index("dp")
    s = lax.axis_index("seq")
    zh, y, c = lax.div(dp, 8), lax.rem(lax.div(dp, 2), 4), lax.rem(dp, 2)
    x, zl = lax.div(s, 4), lax.rem(s, 4)

    def turn(a, o):
        return lax.rem(a + o, 4)

    def at_y(o):
        return {"dp": zh * 8 + turn(y, o) * 2 + c, "seq": s}

    def at_zh(o):
        return {"dp": turn(zh, o) * 8 + y * 2 + c, "seq": s}

    def at_x(o):
        return {"dp": dp, "seq": turn(x, o) * 4 + zl}

    def at_zl(o):
        return {"dp": dp, "seq": x * 4 + turn(zl, o)}

    other = {"dp": zh * 8 + y * 2 + (1 - c), "seq": s}
    after = {"dp": dp, "seq": lax.rem(s + 1, 16)}
    before = {"dp": dp, "seq": lax.rem(s + 15, 16)}

    barrier = pltpu.get_barrier_semaphore()
    peers = [f(o) for f in (at_y, at_zh, at_x, at_zl) for o in (1, 2, 3)]
    peers += [other, after, before]
    offs = (1, 2, 3)

    def at_xy(a, b):
        return {"dp": zh * 8 + turn(y, b) * 2 + c, "seq": turn(x, a) * 4 + zl}

    peers += [at_xy(a, b) for a in offs for b in offs]
    for peer in peers:
        pl.semaphore_signal(
            barrier, inc=1, device_id=peer, device_id_type=pl.DeviceIdType.MESH
        )
    copies = Copies(send_sem, recv_sem)
    copies.someone = other

    pulls = []

    def pull(src, dst):
        pulls.append(pltpu.make_async_copy(src, dst, own_sem.at[len(pulls)]))
        pulls[-1].start()
        return pulls[-1]

    wt_pull = pull(wt_in, wf.at[:, zh, c])
    qkv_pulls = [pull(value_in, value)]
    for h in range(HEADS):
        cols = pl.ds(h * QK, QK)
        qkv_pulls.append(pull(query_in.at[:, cols], qkv.at[h, :, pl.ds(0, QK)]))
        qkv_pulls.append(pull(key_in.at[:, cols], qkv.at[h, :, pl.ds(QK, QK)]))
    feats_pulls = [pull(gain_in, gain), pull(feats_in, fext.at[pl.ds(RIM, ROWS)])]
    rest_pulls = [
        pull(targets_in, targets),
        pull(offsets_in, offsets),
        pull(mask_in, track_mask),
        pull(pairing_in, pairing),
    ]
    rows = C + HEADS * VD
    head_copies = [pull(head_in, head.at[pl.ds(0, rows)])]
    for a in range(4):
        for b in range(4):
            block = head_in.at[pl.ds(256 * b + 64 * a, 64)]
            head_copies.append(pull(block, headp.at[a, pl.ds(64 * b, 64)]))
    fext[0:8, :] = jnp.zeros((8, C), bf16)
    fext[2 * RIM + ROWS - 8 :, :] = jnp.zeros((8, C), bf16)
    head[rows:, :] = jnp.zeros((VP - VD, TRACKS), bf16)

    def columns(o, half):
        if half is None:
            return pl.ds(pl.multiple_of(turn(x, o) * 256, 128), 256)
        return pl.ds(pl.multiple_of(turn(x, o) * 256 + 128 * half, 128), 128)

    def unit_z(o, half):
        if half is None:
            return wf.at[:, turn(zh, o), c, :, :, columns(0, None)]
        return wf.at[:, turn(zh, o), c, half, :, columns(0, None)]

    def unit_yx(r):
        return lambda o, half: wf.at[:, turn(zh, r), c, :, :, columns(o, half)]

    def unit_of(buf):
        def unit(o, half):
            if half is None:
                return buf.at[turn(y, o)]
            return buf.at[turn(y, o), pl.ds(half * 48, 48), :]

        return unit

    kv_cols = pl.ds(QK, 3 * QK)

    def unit_kv(o, half):
        if half is None:
            return kva.at[turn(x, o), :, :, kv_cols]
        return kva.at[turn(x, o), pl.ds(2 * half, 2), :, kv_cols]

    g_z = Gather(copies, at_zh, unit_z)
    g_yx = [Direct(copies, at_x, unit_yx(r)) for r in range(4)]
    g_taps = Gather(copies, at_y, unit_of(taps))
    g_weigh = Gather(copies, at_y, unit_of(weigh))
    g_kv = Direct(copies, at_x, unit_kv)
    wt_pull.wait()
    pl.semaphore_wait(barrier, len(peers))
    for pulled in feats_pulls:
        pulled.wait()
    edge = pl.ds(RIM + ROWS, 8)
    lo = copies.start(fext.at[pl.ds(ROWS + 8, 8)], fext.at[pl.ds(8, 8)], after)
    hi = copies.start(fext.at[pl.ds(RIM, 8)], fext.at[edge], before)
    g_z.begin()
    pair_in = []

    def share(r):
        part = wf.at[:, turn(zh, r), c]
        pair_in.append((copies.start(part, part, other), wf.at[:, turn(zh, r), 1 - c]))

    share(0)

    for pulled in qkv_pulls:
        pulled.wait()
    lane = iota((TOK, VP), 1)
    vals = value[...].astype(f32)
    for h in range(HEADS):
        start = h * VD
        if h % 2 == 0:
            cut = vals[:, start : start + VP]
        else:
            cut = pltpu.roll(vals[:, start - 64 : start + VD], VP - 64, 1)
        qkv[h, :, 2 * QK :] = jnp.where(lane < VD, cut, 0.0).astype(bf16)
    kva[x, zl] = qkv[zl]
    qkv_in = [
        copies.start(qkv.at[turn(zl, o)], kva.at[x, zl], at_zl(o)) for o in offs
    ]
    def pointwise(row):
        at = pl.ds(row, 16)
        f = fext[at, :].astype(f32)
        r = lax.rsqrt(jnp.mean(f * f, axis=1, keepdims=True) + NORM_EPS)
        n = f * r
        g = n * gain[...]
        sq = g * g
        t = jnp.tanh(ROOT * (g + CUBIC * (sq * g)))
        hext[at, :] = (0.5 * g * (1.0 + t)).astype(bf16)
        slope = 0.5 * (1.0 + t) + (0.5 * ROOT) * g * (1.0 - t * t) * (
            1.0 + (3.0 * CUBIC) * sq
        )
        dn = slope * n
        top = dn.astype(bf16)
        dnh[at, :] = top
        dnl[at, :] = (dn - top.astype(f32)).astype(bf16)
        return n, slope, r

    @pl.loop(0, ROWS // 16)
    def _(i):
        row = pl.multiple_of(i * 16, 16)
        n, slope, r = pointwise(pl.multiple_of(row + RIM, 16))
        nbuf[pl.ds(row, 16), :] = n
        dbuf[pl.ds(row, 16), :] = slope * gain[...]
        rbuf[pl.ds(row, 16), :] = jnp.broadcast_to(r, (16, 128))


    for pulled in rest_pulls:
        pulled.wait()
    flip = dp >= PAIRS
    interval = lax.rem(dp, PAIRS)
    sign = jnp.where(flip, -1, 1)
    mine = iota((1, PAIRS), 1) == interval
    chosen = jnp.sum(jnp.where(mine, offsets[...].astype(f32), 0.0), axis=1, keepdims=True)
    off = chosen.astype(jnp.int32) * sign

    EXT = ROWS + 2 * RIM

    def mean_matrix(count, shift_of):
        row, col = iota((count, EXT), 0), iota((count, EXT), 1)
        tok = lax.rem(row, TOK)
        at = col - RIM
        rel = at + off - shift_of(row) - POOL * tok
        where_p = s * ROWS + at + off
        where_q = s * ROWS + at
        fine = (rel >= 0) & (rel < POOL) & (where_p >= 0) & (where_p < L16)
        fine = fine & (where_q >= 0) & (where_q < L16)
        return jnp.where(fine, 1.0 / POOL, 0.0).astype(bf16)

    mix = mean_matrix(KW * TOK, lambda row: (lax.div(row, TOK) - 1) * sign)
    still = mean_matrix(TOK, lambda row: 0 * row)
    copies.arrived(lo, fext.at[pl.ds(8, 8)])
    copies.arrived(hi, fext.at[edge])
    pointwise(0)
    pointwise(RIM + ROWS)
    taps[y] = dot(mix, hext[...], NN).astype(bf16)
    g_taps.begin()
    weigh[y] = ((dot(mix, dnh[...], NN) + dot(mix, dnl[...], NN)) * POOL).astype(bf16)
    pooled_u = dot(still, fext[...], NN).astype(bf16)
    for pulled in head_copies:
        pulled.wait()
    pre[...] = dot(pooled_u, head[0:C, :], NN)

    g_z.relay_from_left()
    g_yx[3].begin()
    g_z.relay_from_right()
    g_yx[1].begin()
    def spread(width, tap_of):
        row, col = iota((ROWS, width), 0), iota((ROWS, width), 1)
        reach = row + off - tap_of(col)
        at = s * ROWS + row + off
        seen = s * ROWS + reach
        fine = (lax.shift_right_arithmetic(reach + 64, 3) == lax.rem(col, 64)) & (at >= 0)
        fine = fine & (at < L16) & (seen >= 0) & (seen < L16)
        return jnp.where(fine, 1.0, 0.0).astype(bf16)

    three[...] = spread(192, lambda col: (lax.div(col, 64) - 1) * sign)
    one[...] = spread(64, lambda col: 0 * col)
    dyt[...] = jnp.zeros((64, C), f32)
    zall[...] = jnp.zeros((KW, 64, C), f32)
    rim_s[...] = jnp.zeros((2, 8, C), f32)

    g_taps.relay()
    g_z.end()
    g_yx[2].begin()
    for o, n in zip(offs, qkv_in):
        copies.arrived(n, kva.at[x, turn(zl, 4 - o)])
    g_kv.begin()
    tgt_s[...] = targets[...].astype(bf16)
    tgt_in = copies.start(tgt_s, tgt_r, at_zh(2))
    g_yx[3].end()
    share(3)
    g_yx[1].end()
    share(1)
    g_taps.end()
    g_yx[2].end()
    share(2)
    g_kv.end()
    inv_sqrt = 1.0 / math.sqrt(QK)
    qh = kva[x, :, :, 0:QK].reshape(4 * TOK, QK)
    kh = kva[:, :, :, QK : 2 * QK].reshape(16 * TOK, QK)
    vh = kva[:, :, :, 2 * QK :].reshape(16 * TOK, VP)
    scores = dot(qh, kh, NT) * inv_sqrt
    e = jnp.exp(scores - jnp.max(scores, axis=1, keepdims=True))
    p = e / jnp.sum(e, axis=1, keepdims=True)
    probs[...] = p
    probs_b[...] = p.astype(bf16)
    att_s[...] = dot(probs_b[...], vh, NN).astype(bf16).reshape(4, TOK, VP)
    att_r[zl] = att_s[zl]
    att_in = [
        copies.start(att_s.at[turn(zl, o)], att_r.at[zl], at_zl(o)) for o in offs
    ]
    for n, part in pair_in:
        copies.arrived(n, part)

    acc = jnp.zeros((4 * TOK, 256), f32)
    for t in range(KW):
        rows_t = taps[:, t * TOK : (t + 1) * TOK, :].reshape(4 * TOK, C)
        acc = acc + dot(rows_t, wf[t].reshape(256, C), NT)
    cv_s[...] = acc.astype(bf16).reshape(4, TOK, 256)
    cv_r[y] = cv_s[y]
    cv_in = [copies.start(cv_s.at[turn(y, o)], cv_r.at[y], at_y(o)) for o in offs]
    g_weigh.begin()
    pick[...] = jnp.where(
        iota((TRACKS, TRACKS), 0) == pairing[...], 1.0, 0.0
    ).astype(bf16)
    mrow = track_mask[pl.ds(interval, 1), :].astype(f32)
    count = jnp.maximum(jnp.sum(mrow, axis=1, keepdims=True), 1.0)
    mpair = dot(jnp.broadcast_to(mrow, (16, TRACKS)).astype(bf16), pick[...], NN)[0:1, :]
    for o, n in zip(offs, att_in):
        copies.arrived(n, att_r.at[turn(zl, 4 - o)])
    for h in range(HEADS):
        pre[...] += dot(att_r[h], head[C + h * VD : C + h * VD + VP, :], NN)
    for o, n in zip(offs, cv_in):
        copies.arrived(n, cv_r.at[turn(y, 4 - o)])

    logits = pre[...]
    for a in range(4):
        logits = logits + dot(cv_r[a], headp[a], NN)
    pred = jnp.maximum(logits, 0.0) + jnp.log1p(jnp.exp(-jnp.abs(logits)))
    pred_s[...] = pred.astype(bf16)
    pred_in = copies.start(pred_s, pred_r, at_zh(2))
    gate = jax.nn.sigmoid(logits)
    copies.arrived(tgt_in, tgt_r)
    tgt_p[...] = dot(tgt_r[...], pick[...], NN)
    g_weigh.relay()
    copies.arrived(pred_in, pred_r)
    both = 0.5 * (pred + dot(pred_r[...], pick[...], NN))
    misfit = both - targets[...]
    weighted = mrow * misfit
    loss = jnp.sum(jnp.sum(weighted * misfit, axis=1, keepdims=True), axis=0, keepdims=True)
    loss = loss / count / (2.0 * PAIRS * TOK * 16)
    dpred = (LOSS_SCALE / count) * (weighted + mpair * (both - tgt_p[...]))
    dlogit = (dpred * gate).astype(bf16)

    for a in range(4):
        part = dot(dlogit, headp[a], NT) * (1.0 / POOL)
        dyp_s[a] = part.astype(bf16)
    dyp_r[y] = dyp_s[y]
    dyp_in = [copies.start(dyp_s.at[turn(y, o)], dyp_r.at[y], at_y(o)) for o in offs]
    for h in range(HEADS):
        part = dot(dlogit, head[C + h * VD : C + h * VD + VP, :], NT)
        datt_s[h] = jnp.where(lane < VD, part, 0.0).astype(bf16)
    datt_r[zl] = datt_s[zl]
    datt_in = [
        copies.start(datt_s.at[turn(zl, o)], datt_r.at[zl], at_zl(o)) for o in offs
    ]
    dyt[8 : 8 + TOK, :] = dot(dlogit, head[0:C, :], NT) * (1.0 / POOL)

    g_weigh.end()
    for o, n in zip(offs, dyp_in):
        copies.arrived(n, dyp_r.at[turn(y, 4 - o)])
    @pl.loop(0, 4)
    def _(b):
        cols = pl.ds(pl.multiple_of(b * 256, 256), 256)
        gains = jnp.zeros((4 * TOK, 256), f32)
        dyr = dyp_r[...].reshape(4 * TOK, 256)
        for t in range(KW):
            part = pl.ds(t * TOK, TOK)
            w = wf[t, :, :, :, :, cols].reshape(256, 256)
            acc = dot(dyr, w, NN)
            zp_s[:, part, cols] = acc.astype(bf16).reshape(4, TOK, 256)
            gains = gains + acc * weigh[:, part, cols].reshape(4 * TOK, 256).astype(f32)
        gacc[:, cols] = jnp.sum(gains, axis=0, keepdims=True)

    zp_in = [copies.start(zp_s.at[turn(y, o)], zp_r.at[y], at_y(o)) for o in offs]
    zp_r[y] = zp_s[y]

    def all_sum(buf, mine, total, device):
        buf[mine] = total
        return [copies.start(buf.at[mine], buf.at[mine], device(o)) for o in offs]

    def sum_of(buf, mine, ins):
        for o, n in zip(offs, ins):
            copies.arrived(n, buf.at[turn(mine, 4 - o)])
        return (buf[0] + buf[1]) + (buf[2] + buf[3])

    ar_c[c] = jnp.concatenate([gacc[...], jnp.broadcast_to(loss, (1, 128))], axis=1)
    ar_in = copies.start(ar_c.at[c], ar_c.at[c], other)
    for o, n in zip(offs, datt_in):
        copies.arrived(n, datt_r.at[turn(zl, 4 - o)])
    dout = datt_r[...].reshape(4 * TOK, VP)
    att = att_s[...].reshape(4 * TOK, VP)
    delta = jnp.sum(dout.astype(f32) * att.astype(f32), axis=1, keepdims=True)
    vh = kva[:, :, :, 2 * QK :].reshape(16 * TOK, VP)
    ds = (probs[...] * (dot(dout, vh, NT) - delta)).astype(bf16)
    qh = kva[x, :, :, 0:QK].reshape(4 * TOK, QK)
    kvp_s[:, :, :, 0:QK] = dot(ds, qh, TN).astype(bf16).reshape(4, 4, TOK, QK)
    kvp_s[:, :, :, QK:] = dot(probs_b[...], dout, TN).astype(bf16).reshape(4, 4, TOK, VP)
    kvp_in = [copies.start(kvp_s.at[turn(x, o)], kvp_r.at[x], at_x(o)) for o in offs]
    kh = kva[:, :, :, QK : 2 * QK].reshape(16 * TOK, QK)
    dq_s[...] = (dot(ds, kh, NN) * inv_sqrt).astype(bf16).reshape(4, TOK, QK)
    dq_r[zl] = dq_s[zl]
    dq_in = [copies.start(dq_s.at[turn(zl, o)], dq_r.at[zl], at_zl(o)) for o in offs]
    copies.arrived(ar_in, ar_c.at[1 - c])
    ar_in = all_sum(ar_h, zh, ar_c[0] + ar_c[1], at_zh)

    for o, n in zip(offs, kvp_in):
        copies.arrived(n, kvp_r.at[turn(x, 4 - o)])
    total = kvp_s[x].astype(f32)
    for o in offs:
        total = total + kvp_r[turn(x, o)].astype(f32)
    kvg_s[:, :, 0:QK] = (total[:, :, 0:QK] * inv_sqrt).astype(bf16)
    kvg_s[:, :, QK:] = total[:, :, QK:].astype(bf16)
    kvg_r[zl] = kvg_s[zl]
    kvg_in = [
        copies.start(kvg_s.at[turn(zl, o)], kvg_r.at[zl], at_zl(o)) for o in offs
    ]
    ar_in = all_sum(ar_l, zl, sum_of(ar_h, zh, ar_in), at_zl)
    for o, n in zip(offs, zp_in):
        copies.arrived(n, zp_r.at[turn(y, 4 - o)])

    @pl.loop(0, 4)
    def _(b):
        cols = pl.ds(pl.multiple_of(b * 256, 256), 256)
        for t in range(KW):
            part = pl.ds(t * TOK, TOK)
            low = zp_r[0, part, cols].astype(f32) + zp_r[1, part, cols].astype(f32)
            high = zp_r[2, part, cols].astype(f32) + zp_r[3, part, cols].astype(f32)
            zall[t, 8 : 8 + TOK, cols] = low + high

    for t in range(KW):
        rim_s[0, t : t + 1, :] = zall[t, 8:9, :]
        rim_s[1, t : t + 1, :] = zall[t, 7 + TOK : 8 + TOK, :]
    rim_s[0, KW : KW + 1, :] = dyt[8:9, :]
    rim_s[1, KW : KW + 1, :] = dyt[7 + TOK : 8 + TOK, :]
    rim_hi = copies.start(rim_s.at[0], rim_r.at[0], before)
    rim_lo = copies.start(rim_s.at[1], rim_r.at[1], after)
    copies.arrived(rim_hi, rim_r.at[0])
    copies.arrived(rim_lo, rim_r.at[1])
    ar_p[x, y] = sum_of(ar_l, zl, ar_in)
    plane = [(a, b) for a in range(4) for b in range(4) if a or b]
    ar_in = [
        copies.start(ar_p.at[x, y], ar_p.at[x, y], at_xy(a, b)) for a, b in plane
    ]
    for t in range(KW):
        zall[t, 7:8, :] = rim_r[1, t : t + 1, :]
        zall[t, 8 + TOK : 9 + TOK, :] = rim_r[0, t : t + 1, :]
    dyt[7:8, :] = rim_r[1, KW : KW + 1, :]
    dyt[8 + TOK : 9 + TOK, :] = rim_r[0, KW : KW + 1, :]

    @pl.loop(0, 4)
    def _(b):
        cols = pl.ds(pl.multiple_of(b * 256, 256), 256)

        def exact(mat, val):
            top = val.astype(bf16)
            low = (val - top.astype(f32)).astype(bf16)
            return dot(mat, top, NN) + dot(mat, low, NN)

        dhb[:, cols] = exact(three[...], zall[:, :, cols].reshape(KW * 64, 256))
        dyb[:, cols] = exact(one[...], dyt[:, cols])

    @pl.loop(0, ROWS // 16)
    def _(i):
        at = pl.ds(pl.multiple_of(i * 16, 16), 16)
        n = nbuf[at, :]
        dn = dhb[at, :] * dbuf[at, :]
        mid = jnp.mean(dn * n, axis=1, keepdims=True)
        r = rbuf[at, :][:, 0:1]
        dfeats[at, :] = (r * (dn - n * mid) + dyb[at, :]).astype(bf16)

    for o, n in zip(offs, dq_in):
        copies.arrived(n, dq_r.at[turn(zl, 4 - o)])
    for h in range(HEADS):
        dquery[:, h * QK : (h + 1) * QK] = dq_r[h]
    for o, n in zip(offs, kvg_in):
        copies.arrived(n, kvg_r.at[turn(zl, 4 - o)])
    for h in range(HEADS):
        dkey[:, h * QK : (h + 1) * QK] = kvg_r[h, :, 0:QK]
    for h in (0, 2):
        even = kvg_r[h, :, QK:].astype(f32)
        odd = pltpu.roll(kvg_r[h + 1, :, QK:].astype(f32), VD, 1)
        start = h * VD
        dvalue[:, start : start + VP] = jnp.where(lane < VD, even, odd).astype(bf16)
        dvalue[:, start + VP : start + VP + 128] = odd[:, 0:128].astype(bf16)

    for (a, b), n in zip(plane, ar_in):
        copies.arrived(n, ar_p.at[turn(x, 4 - a), turn(y, 4 - b)])
    total = jnp.zeros((1, ROW), f32)
    for a in range(4):
        total = total + ((ar_p[a, 0] + ar_p[a, 1]) + (ar_p[a, 2] + ar_p[a, 3]))
    dgain[...] = total[:, 0:C]
    loss_out[...] = total[:, C:]
    copies.finish()


def store_kernel(*refs):
    sems = refs[12]
    puts = [pltpu.make_async_copy(refs[i], refs[6 + i], sems.at[i]) for i in range(6)]
    for put in puts:
        put.start()
    for put in puts:
        put.wait()


def body(
    features,
    shift_offsets,
    conv_weight,
    norm_gain,
    query_proj,
    key_proj,
    value_proj,
    head_weight,
    targets,
    track_mask,
    track_pairing,
):
    wt = jnp.swapaxes(conv_weight, 1, 2).reshape(KW, 2, 16, C)
    vmem = pl.BlockSpec(memory_space=pltpu.VMEM)
    hbm = pl.BlockSpec(memory_space=pltpu.HBM)
    V = pltpu.VMEM
    scratch = [
        V((1, PAIRS), jnp.int32),
        V((1, C), f32),
        V((TOK, HEADS * VD), bf16),
        V((TOK, TRACKS), f32),
        V((PAIRS, TRACKS), jnp.int32),
        V((1, TRACKS), jnp.int32),
        V((KW, 4, 2, 2, 16, C), bf16),
        V((ROWS + 2 * RIM, C), bf16),
        V((ROWS + 2 * RIM, C), bf16),
        V((ROWS + 2 * RIM, C), bf16),
        V((ROWS + 2 * RIM, C), bf16),
        V((ROWS, C), f32),
        V((ROWS, C), f32),
        V((ROWS, 128), f32),
        V((C + HEADS * VD + VP - VD, TRACKS), bf16),
        V((4, 256, TRACKS), bf16),
        V((4, TOK, 512), bf16),
        V((4, 4, TOK, 512), bf16),
        V((4, TOK, VP), bf16),
        V((4, TOK, VP), bf16),
        V((4 * TOK, 16 * TOK), f32),
        V((4 * TOK, 16 * TOK), bf16),
        V((4, KW * TOK, C), bf16),
        V((4, KW * TOK, C), bf16),
        V((4, TOK, 256), bf16),
        V((4, TOK, 256), bf16),
        V((4, TOK, 256), bf16),
        V((4, TOK, 256), bf16),
        V((4, KW * TOK, C), bf16),
        V((4, KW * TOK, C), bf16),
        V((TOK, TRACKS), f32),
        V((TOK, TRACKS), bf16),
        V((TOK, TRACKS), bf16),
        V((TOK, TRACKS), bf16),
        V((TOK, TRACKS), bf16),
        V((TRACKS, TRACKS), bf16),
        V((TOK, TRACKS), f32),
        V((ROWS, KW * 64), bf16),
        V((ROWS, 64), bf16),
        V((4, TOK, VP), bf16),
        V((4, TOK, VP), bf16),
        V((4, TOK, QK), bf16),
        V((4, TOK, QK), bf16),
        V((4, 4, TOK, 384), bf16),
        V((4, 4, TOK, 384), bf16),
        V((4, TOK, 384), bf16),
        V((4, TOK, 384), bf16),
        V((64, C), f32),
        V((KW, 64, C), f32),
        V((2, 8, C), f32),
        V((2, 8, C), f32),
        V((ROWS, C), f32),
        V((ROWS, C), f32),
        V((1, C), f32),
        V((2, 1, ROW), f32),
        V((4, 4, 1, ROW), f32),
        V((4, 1, ROW), f32),
        V((4, 1, ROW), f32),
        pltpu.SemaphoreType.DMA((COPIES,)),
        pltpu.SemaphoreType.DMA((COPIES,)),
        pltpu.SemaphoreType.DMA((36,)),
    ]
    out = jax.ShapeDtypeStruct
    outs = pl.pallas_call(
        step_kernel,
        name="strand_step",
        out_shape=(
            out((ROWS, C), bf16),
            out((TOK, HEADS * QK), bf16),
            out((TOK, HEADS * QK), bf16),
            out((TOK, HEADS * VD), bf16),
            out((1, C), f32),
            out((1, 128), f32),
        ),
        in_specs=[hbm] * 11,
        out_specs=(vmem,) * 6,
        scratch_shapes=scratch,
        compiler_params=pltpu.CompilerParams(
            collective_id=0, has_side_effects=True, vmem_limit_bytes=48 << 20
        ),
    )(
        *(
            pltpu.with_memory_space_constraint(a, pltpu.HBM)
            for a in (
                features[0],
                shift_offsets.reshape(1, PAIRS),
                wt,
                norm_gain.reshape(1, C),
                query_proj[0],
                key_proj[0],
                value_proj[0],
                head_weight,
                targets[0],
                track_mask,
                track_pairing.reshape(1, TRACKS),
            )
        )
    )
    outs = pl.pallas_call(
        store_kernel,
        name="store",
        out_shape=tuple(out(o.shape, o.dtype) for o in outs),
        in_specs=[vmem] * 6,
        out_specs=(hbm,) * 6,
        scratch_shapes=[pltpu.SemaphoreType.DMA((6,))],
        compiler_params=pltpu.CompilerParams(vmem_limit_bytes=4 << 20),
    )(*outs)
    features_grad, query_grad, key_grad, value_grad, gain_grad, loss = outs
    return (
        features_grad[None],
        query_grad[None],
        key_grad[None],
        value_grad[None],
        gain_grad.reshape(C),
        loss[0, 0],
    )


def solution(mesh):
    placed = (
        P("dp", "seq", None),
        P(),
        P(None, None, "dp"),
        P(),
        P("dp", "seq", None),
        P("dp", "seq", None),
        P("dp", "seq", None),
        P(),
        P("dp", "seq", None),
        P(),
        P(),
    )
    return jax.shard_map(
        body,
        mesh=mesh,
        in_specs=placed,
        out_specs=(
            P("dp", "seq", None),
            P("dp", "seq", None),
            P("dp", "seq", None),
            P("dp", "seq", None),
            P(),
            P(),
        ),
        check_vma=False,
    )
```

```python
import math

import jax
import jax.numpy as jnp
from jax import lax
from jax.experimental import pallas as pl
from jax.experimental.pallas import tpu as pltpu
from jax.sharding import PartitionSpec as P

KW = 3
SHIFT = 4
POOL = 8
HEADS = 4
QK = 128
VD = 192
C = 1024
TRACKS = 512
ROWS = 256
TOK = 32
L16 = 4096
PAIRS = 16
RIM = 16
VP = 256
ROW = 1152
NORM_EPS = 1e-06
LOSS_SCALE = 1024.0
ROOT = math.sqrt(2.0 / math.pi)
CUBIC = 0.044715
COPIES = 121
f32 = jnp.float32
bf16 = jnp.bfloat16

NT = (((1,), (1,)), ((), ()))
NN = (((1,), (0,)), ((), ()))
TN = (((0,), (0,)), ((), ()))


def dot(a, b, dims):
    return lax.dot_general(a, b, dims, preferred_element_type=f32)


def iota(shape, axis):
    return lax.broadcasted_iota(jnp.int32, shape, axis)


class Copies:
    def __init__(self, send, recv):
        self.send, self.recv, self.used, self.sent = send, recv, 0, []

    def start(self, src, dst, device):
        n = self.used
        self.used += 1
        copy = pltpu.make_async_remote_copy(
            src_ref=src,
            dst_ref=dst,
            send_sem=self.send.at[n],
            recv_sem=self.recv.at[n],
            device_id=device,
            device_id_type=pl.DeviceIdType.MESH,
        )
        copy.start()
        self.sent.append(copy)
        return n

    def arrived(self, n, dst):
        pltpu.make_async_remote_copy(
            src_ref=dst,
            dst_ref=dst,
            send_sem=self.send.at[n],
            recv_sem=self.recv.at[n],
            device_id=self.someone,
            device_id_type=pl.DeviceIdType.MESH,
        ).wait_recv()

    def finish(self):
        assert self.used <= COPIES
        for copy in self.sent:
            copy.wait_send()


class Gather:
    def __init__(self, copies, device, unit):
        self.copies, self.device, self.unit = copies, device, unit

    def begin(self):
        mine = self.unit(0, None)
        self.right = self.copies.start(mine, mine, self.device(1))
        self.left = self.copies.start(mine, mine, self.device(3))

    def relay_from_left(self):
        self.copies.arrived(self.right, self.unit(3, None))
        part = self.unit(3, 0)
        self.far_right = self.copies.start(part, part, self.device(1))

    def relay_from_right(self):
        self.copies.arrived(self.left, self.unit(1, None))
        part = self.unit(1, 1)
        self.far_left = self.copies.start(part, part, self.device(3))

    def relay(self):
        self.relay_from_left()
        self.relay_from_right()

    def end(self):
        self.copies.arrived(self.far_right, self.unit(2, 0))
        self.copies.arrived(self.far_left, self.unit(2, 1))


class Direct(Gather):
    def begin(self):
        mine = self.unit(0, None)
        self.ins = [(o, self.copies.start(mine, mine, self.device(o))) for o in (1, 3, 2)]

    def end(self):
        for o, n in self.ins:
            self.copies.arrived(n, self.unit(4 - o, None))


def step_kernel(
    feats_in,
    offsets_in,
    wt_in,
    gain_in,
    query_in,
    key_in,
    value_in,
    head_in,
    targets_in,
    mask_in,
    pairing_in,
    dfeats,
    dquery,
    dkey,
    dvalue,
    dgain,
    loss_out,
    offsets,
    gain,
    value,
    targets,
    track_mask,
    pairing,
    wf,
    fext,
    hext,
    dnh,
    dnl,
    nbuf,
    dbuf,
    rbuf,
    head,
    headp,
    qkv,
    kva,
    att_s,
    att_r,
    probs,
    probs_b,
    taps,
    weigh,
    cv_s,
    cv_r,
    dyp_s,
    dyp_r,
    zp_s,
    zp_r,
    pre,
    pred_s,
    pred_r,
    tgt_s,
    tgt_r,
    pick,
    tgt_p,
    three,
    one,
    datt_s,
    datt_r,
    dq_s,
    dq_r,
    kvp_s,
    kvp_r,
    kvg_s,
    kvg_r,
    dyt,
    zall,
    rim_s,
    rim_r,
    dhb,
    dyb,
    gacc,
    ar_c,
    ar_p,
    ar_z,
    send_sem,
    recv_sem,
    own_sem,
):
    dp = lax.axis_index("dp")
    s = lax.axis_index("seq")
    zh, y, c = lax.div(dp, 8), lax.rem(lax.div(dp, 2), 4), lax.rem(dp, 2)
    x, zl = lax.div(s, 4), lax.rem(s, 4)

    def turn(a, o):
        return lax.rem(a + o, 4)

    def at_y(o):
        return {"dp": zh * 8 + turn(y, o) * 2 + c, "seq": s}

    def at_zh(o):
        return {"dp": turn(zh, o) * 8 + y * 2 + c, "seq": s}

    def at_x(o):
        return {"dp": dp, "seq": turn(x, o) * 4 + zl}

    def at_zl(o):
        return {"dp": dp, "seq": x * 4 + turn(zl, o)}

    other = {"dp": zh * 8 + y * 2 + (1 - c), "seq": s}
    after = {"dp": dp, "seq": lax.rem(s + 1, 16)}
    before = {"dp": dp, "seq": lax.rem(s + 15, 16)}

    barrier = pltpu.get_barrier_semaphore()
    peers = [f(o) for f in (at_y, at_x, at_zl) for o in (1, 2, 3)]
    peers += [at_zh(1), at_zh(3)]
    peers += [other, after, before]
    offs = (1, 2, 3)

    def at_xy(a, b):
        return {"dp": zh * 8 + turn(y, b) * 2 + c, "seq": turn(x, a) * 4 + zl}

    peers += [at_xy(a, b) for a in offs for b in offs]

    def around(o):
        return lax.rem(zh * 4 + zl + o, 16)

    def at_z(o):
        z = around(o)
        return {"dp": lax.div(z, 4) * 8 + y * 2 + c, "seq": x * 4 + lax.rem(z, 4)}
    for peer in peers:
        pl.semaphore_signal(
            barrier, inc=1, device_id=peer, device_id_type=pl.DeviceIdType.MESH
        )
    copies = Copies(send_sem, recv_sem)
    copies.someone = other

    pulls = []

    def pull(src, dst):
        pulls.append(pltpu.make_async_copy(src, dst, own_sem.at[len(pulls)]))
        pulls[-1].start()
        return pulls[-1]

    wt_pull = pull(wt_in, wf.at[:, 0, c])
    qkv_pulls = [pull(value_in, value)]
    for h in range(HEADS):
        cols = pl.ds(h * QK, QK)
        qkv_pulls.append(pull(query_in.at[:, cols], qkv.at[h, :, pl.ds(0, QK)]))
        qkv_pulls.append(pull(key_in.at[:, cols], qkv.at[h, :, pl.ds(QK, QK)]))
    feats_pulls = [pull(gain_in, gain), pull(feats_in, fext.at[pl.ds(RIM, ROWS)])]
    rest_pulls = [
        pull(targets_in, targets),
        pull(offsets_in, offsets),
        pull(mask_in, track_mask),
        pull(pairing_in, pairing),
    ]
    rows = C + HEADS * VD
    head_copies = [pull(head_in, head.at[pl.ds(0, rows)])]
    for a in range(4):
        for b in range(4):
            start = pl.multiple_of(256 * turn(zh, b) + 64 * a, 64)
            block = head_in.at[pl.ds(start, 64)]
            head_copies.append(pull(block, headp.at[a, pl.ds(64 * b, 64)]))
    fext[0:8, :] = jnp.zeros((8, C), bf16)
    fext[2 * RIM + ROWS - 8 :, :] = jnp.zeros((8, C), bf16)
    head[rows:, :] = jnp.zeros((VP - VD, TRACKS), bf16)

    def columns(o, half):
        if half is None:
            return pl.ds(pl.multiple_of(turn(x, o) * 256, 128), 256)
        return pl.ds(pl.multiple_of(turn(x, o) * 256 + 128 * half, 128), 128)

    def slot(t, r, half):
        if half is None:
            return wf.at[t, r, c, :, :, columns(0, None)]
        return wf.at[t, r, c, half, :, columns(0, None)]

    def unit_yx(t, r):
        return lambda o, half: wf.at[t, r, c, :, :, columns(o, half)]

    def unit_of(buf):
        def unit(o, half):
            if half is None:
                return buf.at[turn(y, o)]
            return buf.at[turn(y, o), pl.ds(half * 48, 48), :]

        return unit

    kv_cols = pl.ds(QK, 3 * QK)

    def unit_kv(o, half):
        if half is None:
            return kva.at[turn(x, o), :, :, kv_cols]
        return kva.at[turn(x, o), pl.ds(2 * half, 2), :, kv_cols]

    g_yx = [[Direct(copies, at_x, unit_yx(t, r)) for r in range(4)] for t in range(KW)]
    g_taps = Gather(copies, at_y, unit_of(taps))
    g_weigh = Gather(copies, at_y, unit_of(weigh))
    g_kv = Direct(copies, at_x, unit_kv)
    wt_pull.wait()
    pl.semaphore_wait(barrier, len(peers))
    for pulled in feats_pulls:
        pulled.wait()
    edge = pl.ds(RIM + ROWS, 8)
    lo = copies.start(fext.at[pl.ds(ROWS + 8, 8)], fext.at[pl.ds(8, 8)], after)
    hi = copies.start(fext.at[pl.ds(RIM, 8)], fext.at[edge], before)
    z_in = []
    for t in range(KW):
        right = copies.start(slot(t, 0, None), slot(t, 3, None), at_zh(1))
        left = copies.start(slot(t, 0, None), slot(t, 1, None), at_zh(3))
        z_in.append((right, left))
    pair_in = []

    def share(r, t=None):
        taps_of = pl.ds(0, KW) if t is None else t
        part = wf.at[taps_of, r, c]
        n = copies.start(part, part, other)
        pair_in.append((r, n, wf.at[taps_of, r, 1 - c]))

    share(0)

    for pulled in qkv_pulls:
        pulled.wait()
    lane = iota((TOK, VP), 1)
    vals = value[...].astype(f32)
    for h in range(HEADS):
        start = h * VD
        if h % 2 == 0:
            cut = vals[:, start : start + VP]
        else:
            cut = pltpu.roll(vals[:, start - 64 : start + VD], VP - 64, 1)
        qkv[h, :, 2 * QK :] = jnp.where(lane < VD, cut, 0.0).astype(bf16)
    kva[x, zl] = qkv[zl]
    qkv_in = [
        copies.start(qkv.at[turn(zl, o)], kva.at[x, zl], at_zl(o)) for o in offs
    ]
    def normed(row):
        f = fext[pl.ds(row, 16), :].astype(f32)
        r = lax.rsqrt(jnp.mean(f * f, axis=1, keepdims=True) + NORM_EPS)
        n = f * r
        g = n * gain[...]
        sq = g * g
        t = jnp.tanh(ROOT * (g + CUBIC * (sq * g)))
        return n, g, sq, t, r

    def hidden(row):
        n, g, sq, t, r = normed(row)
        hext[pl.ds(row, 16), :] = (0.5 * g * (1.0 + t)).astype(bf16)

    def slopes(row):
        n, g, sq, t, r = normed(row)
        slope = 0.5 * (1.0 + t) + (0.5 * ROOT) * g * (1.0 - t * t) * (
            1.0 + (3.0 * CUBIC) * sq
        )
        dn = slope * n
        top = dn.astype(bf16)
        dnh[pl.ds(row, 16), :] = top
        dnl[pl.ds(row, 16), :] = (dn - top.astype(f32)).astype(bf16)
        return n, slope, r

    @pl.loop(1, 1 + ROWS // 16)
    def _(i):
        hidden(pl.multiple_of(i * 16, 16))

    for pulled in rest_pulls:
        pulled.wait()
    flip = dp >= PAIRS
    interval = lax.rem(dp, PAIRS)
    sign = jnp.where(flip, -1, 1)
    mine = iota((1, PAIRS), 1) == interval
    chosen = jnp.sum(jnp.where(mine, offsets[...].astype(f32), 0.0), axis=1, keepdims=True)
    off = chosen.astype(jnp.int32) * sign

    EXT = ROWS + 2 * RIM

    def mean_matrix(count, shift_of):
        row, col = iota((count, EXT), 0), iota((count, EXT), 1)
        tok = lax.rem(row, TOK)
        at = col - RIM
        rel = at + off - shift_of(row) - POOL * tok
        where_p = s * ROWS + at + off
        where_q = s * ROWS + at
        fine = (rel >= 0) & (rel < POOL) & (where_p >= 0) & (where_p < L16)
        fine = fine & (where_q >= 0) & (where_q < L16)
        return jnp.where(fine, 1.0 / POOL, 0.0).astype(bf16)

    mix = mean_matrix(KW * TOK, lambda row: (lax.div(row, TOK) - 1) * sign)
    still = mean_matrix(TOK, lambda row: 0 * row)
    copies.arrived(lo, fext.at[pl.ds(8, 8)])
    copies.arrived(hi, fext.at[edge])
    hidden(0)
    hidden(RIM + ROWS)
    taps[y] = dot(mix, hext[...], NN).astype(bf16)
    g_taps.begin()
    pooled_u = dot(still, fext[...], NN).astype(bf16)

    def later(first, last):
        @pl.loop(first, last)
        def _(i):
            row = pl.multiple_of(i * 16, 16)
            n, slope, r = slopes(pl.multiple_of(row + RIM, 16))
            nbuf[pl.ds(row, 16), :] = n
            dbuf[pl.ds(row, 16), :] = slope * gain[...]
            rbuf[pl.ds(row, 16), :] = jnp.broadcast_to(r, (16, 128))

    z_far = []
    for t in range(KW):
        right, left = z_in[t]
        copies.arrived(right, slot(t, 3, None))
        to_right = copies.start(slot(t, 3, 0), slot(t, 2, 0), at_zh(1))
        g_yx[t][3].begin()
        copies.arrived(left, slot(t, 1, None))
        to_left = copies.start(slot(t, 1, 1), slot(t, 2, 1), at_zh(3))
        g_yx[t][1].begin()
        z_far.append((to_right, to_left))
    for o, n in zip(offs, qkv_in):
        copies.arrived(n, kva.at[x, turn(zl, 4 - o)])
    g_kv.begin()
    g_taps.relay()
    for pulled in head_copies:
        pulled.wait()
    pre[...] = dot(pooled_u, head[0:C, :], NN)
    def spread(width, tap_of):
        row, col = iota((ROWS, width), 0), iota((ROWS, width), 1)
        reach = row + off - tap_of(col)
        at = s * ROWS + row + off
        seen = s * ROWS + reach
        fine = (lax.shift_right_arithmetic(reach + 64, 3) == lax.rem(col, 64)) & (at >= 0)
        fine = fine & (at < L16) & (seen >= 0) & (seen < L16)
        return jnp.where(fine, 1.0, 0.0).astype(bf16)

    three[...] = spread(192, lambda col: (lax.div(col, 64) - 1) * sign)
    one[...] = spread(64, lambda col: 0 * col)
    dyt[...] = jnp.zeros((64, C), f32)
    zall[...] = jnp.zeros((KW, 64, C), f32)
    rim_s[...] = jnp.zeros((2, 8, C), f32)

    later(0, 8)
    for t in range(KW):
        to_right, to_left = z_far[t]
        copies.arrived(to_right, slot(t, 2, 0))
        copies.arrived(to_left, slot(t, 2, 1))
        g_yx[t][2].begin()
    tgt_s[...] = targets[...].astype(bf16)
    tgt_in = copies.start(tgt_s, tgt_r, at_zh(2))
    for r in (3, 1):
        for t in range(KW):
            g_yx[t][r].end()
        share(r)
    slopes(0)
    slopes(RIM + ROWS)
    later(8, 16)
    g_taps.end()

    def convolve(r):
        for q, n, part in pair_in:
            if q == r:
                copies.arrived(n, part)
        acc = jnp.zeros((4 * TOK, 64), f32)
        for t in range(KW):
            rows_t = taps[:, t * TOK : (t + 1) * TOK, :].reshape(4 * TOK, C)
            acc = acc + dot(rows_t, wf[t, r].reshape(64, C), NT)
        cv_s[:, :, r * 64 : (r + 1) * 64] = acc.astype(bf16).reshape(4, TOK, 64)

    convolve(0)
    g_kv.end()
    inv_sqrt = 1.0 / math.sqrt(QK)
    qh = kva[x, :, :, 0:QK].reshape(4 * TOK, QK)
    kh = kva[:, :, :, QK : 2 * QK].reshape(16 * TOK, QK)
    vh = kva[:, :, :, 2 * QK :].reshape(16 * TOK, VP)
    scores = dot(qh, kh, NT) * inv_sqrt
    e = jnp.exp(scores - jnp.max(scores, axis=1, keepdims=True))
    p = e / jnp.sum(e, axis=1, keepdims=True)
    probs[...] = p
    probs_b[...] = p.astype(bf16)
    att_s[...] = dot(probs_b[...], vh, NN).astype(bf16).reshape(4, TOK, VP)
    att_r[zl] = att_s[zl]
    att_in = [
        copies.start(att_s.at[turn(zl, o)], att_r.at[zl], at_zl(o)) for o in offs
    ]
    for t in range(KW):
        g_yx[t][2].end()
        share(2, t)
    convolve(3)
    convolve(1)
    convolve(2)
    cv_r[y] = cv_s[y]
    cv_in = [copies.start(cv_s.at[turn(y, o)], cv_r.at[y], at_y(o)) for o in offs]
    both = dot(mix, dnh[...], NN) + dot(mix, dnl[...], NN)
    weigh[y] = (both * POOL).astype(bf16)
    g_weigh.begin()
    pick[...] = jnp.where(
        iota((TRACKS, TRACKS), 0) == pairing[...], 1.0, 0.0
    ).astype(bf16)
    mrow = track_mask[pl.ds(interval, 1), :].astype(f32)
    count = jnp.maximum(jnp.sum(mrow, axis=1, keepdims=True), 1.0)
    mpair = dot(jnp.broadcast_to(mrow, (16, TRACKS)).astype(bf16), pick[...], NN)[0:1, :]
    for o, n in zip(offs, att_in):
        copies.arrived(n, att_r.at[turn(zl, 4 - o)])
    for h in range(HEADS):
        pre[...] += dot(att_r[h], head[C + h * VD : C + h * VD + VP, :], NN)
    for o, n in zip(offs, cv_in):
        copies.arrived(n, cv_r.at[turn(y, 4 - o)])

    logits = pre[...]
    for a in range(4):
        logits = logits + dot(cv_r[a], headp[a], NN)
    pred = jnp.maximum(logits, 0.0) + jnp.log1p(jnp.exp(-jnp.abs(logits)))
    pred_s[...] = pred.astype(bf16)
    pred_in = copies.start(pred_s, pred_r, at_zh(2))
    gate = jax.nn.sigmoid(logits)
    copies.arrived(tgt_in, tgt_r)
    tgt_p[...] = dot(tgt_r[...], pick[...], NN)
    g_weigh.relay()
    copies.arrived(pred_in, pred_r)
    both = 0.5 * (pred + dot(pred_r[...], pick[...], NN))
    misfit = both - targets[...]
    weighted = mrow * misfit
    dpred = (LOSS_SCALE / count) * (weighted + mpair * (both - tgt_p[...]))
    dlogit = (dpred * gate).astype(bf16)

    for a in range(4):
        part = dot(dlogit, headp[a], NT) * (1.0 / POOL)
        dyp_s[a] = part.astype(bf16)
    dyp_r[y] = dyp_s[y]
    dyp_in = [copies.start(dyp_s.at[turn(y, o)], dyp_r.at[y], at_y(o)) for o in offs]
    for h in range(HEADS):
        part = dot(dlogit, head[C + h * VD : C + h * VD + VP, :], NT)
        datt_s[h] = jnp.where(lane < VD, part, 0.0).astype(bf16)
    datt_r[zl] = datt_s[zl]
    datt_in = [
        copies.start(datt_s.at[turn(zl, o)], datt_r.at[zl], at_zl(o)) for o in offs
    ]
    dyt[8 : 8 + TOK, :] = dot(dlogit, head[0:C, :], NT) * (1.0 / POOL)

    loss = jnp.sum(jnp.sum(weighted * misfit, axis=1, keepdims=True), axis=0, keepdims=True)
    loss = loss / count / (2.0 * PAIRS * TOK * 16)
    g_weigh.end()
    for o, n in zip(offs, dyp_in):
        copies.arrived(n, dyp_r.at[turn(y, 4 - o)])
    @pl.loop(0, 4)
    def _(b):
        cols = pl.ds(pl.multiple_of(b * 256, 256), 256)
        gains = jnp.zeros((4 * TOK, 256), f32)
        dyr = dyp_r[...].reshape(4 * TOK, 256)
        for t in range(KW):
            part = pl.ds(t * TOK, TOK)
            w = wf[t, :, :, :, :, cols].reshape(256, 256)
            acc = dot(dyr, w, NN)
            zp_s[:, part, cols] = acc.astype(bf16).reshape(4, TOK, 256)
            gains = gains + acc * weigh[:, part, cols].reshape(4 * TOK, 256).astype(f32)
        gacc[:, cols] = jnp.sum(gains, axis=0, keepdims=True)

    zp_in = [copies.start(zp_s.at[turn(y, o)], zp_r.at[y], at_y(o)) for o in offs]
    zp_r[y] = zp_s[y]

    ar_c[c] = jnp.concatenate([gacc[...], jnp.broadcast_to(loss, (1, 128))], axis=1)
    ar_in = copies.start(ar_c.at[c], ar_c.at[c], other)
    for o, n in zip(offs, datt_in):
        copies.arrived(n, datt_r.at[turn(zl, 4 - o)])
    dout = datt_r[...].reshape(4 * TOK, VP)
    att = att_s[...].reshape(4 * TOK, VP)
    delta = jnp.sum(dout.astype(f32) * att.astype(f32), axis=1, keepdims=True)
    vh = kva[:, :, :, 2 * QK :].reshape(16 * TOK, VP)
    ds = (probs[...] * (dot(dout, vh, NT) - delta)).astype(bf16)
    qh = kva[x, :, :, 0:QK].reshape(4 * TOK, QK)
    kvp_s[:, :, :, 0:QK] = dot(ds, qh, TN).astype(bf16).reshape(4, 4, TOK, QK)
    kvp_s[:, :, :, QK:] = dot(probs_b[...], dout, TN).astype(bf16).reshape(4, 4, TOK, VP)
    kvp_in = [copies.start(kvp_s.at[turn(x, o)], kvp_r.at[x], at_x(o)) for o in offs]
    kh = kva[:, :, :, QK : 2 * QK].reshape(16 * TOK, QK)
    dq_s[...] = (dot(ds, kh, NN) * inv_sqrt).astype(bf16).reshape(4, TOK, QK)
    dq_r[zl] = dq_s[zl]
    dq_in = [copies.start(dq_s.at[turn(zl, o)], dq_r.at[zl], at_zl(o)) for o in offs]
    copies.arrived(ar_in, ar_c.at[1 - c])
    ar_z[around(0)] = ar_c[0] + ar_c[1]
    ring = (8, 7, 9, 6, 10, 5, 11, 4, 12, 3, 13, 2, 14, 1, 15)
    ar_in = [copies.start(ar_z.at[around(0)], ar_z.at[around(0)], at_z(o)) for o in ring]

    for o, n in zip(offs, kvp_in):
        copies.arrived(n, kvp_r.at[turn(x, 4 - o)])
    total = kvp_s[x].astype(f32)
    for o in offs:
        total = total + kvp_r[turn(x, o)].astype(f32)
    kvg_s[:, :, 0:QK] = (total[:, :, 0:QK] * inv_sqrt).astype(bf16)
    kvg_s[:, :, QK:] = total[:, :, QK:].astype(bf16)
    kvg_r[zl] = kvg_s[zl]
    kvg_in = [
        copies.start(kvg_s.at[turn(zl, o)], kvg_r.at[zl], at_zl(o)) for o in offs
    ]
    for o, n in zip(offs, zp_in):
        copies.arrived(n, zp_r.at[turn(y, 4 - o)])

    @pl.loop(0, 4)
    def _(b):
        cols = pl.ds(pl.multiple_of(b * 256, 256), 256)
        for t in range(KW):
            part = pl.ds(t * TOK, TOK)
            low = zp_r[0, part, cols].astype(f32) + zp_r[1, part, cols].astype(f32)
            high = zp_r[2, part, cols].astype(f32) + zp_r[3, part, cols].astype(f32)
            zall[t, 8 : 8 + TOK, cols] = low + high

    for t in range(KW):
        rim_s[0, t : t + 1, :] = zall[t, 8:9, :]
        rim_s[1, t : t + 1, :] = zall[t, 7 + TOK : 8 + TOK, :]
    rim_s[0, KW : KW + 1, :] = dyt[8:9, :]
    rim_s[1, KW : KW + 1, :] = dyt[7 + TOK : 8 + TOK, :]
    rim_hi = copies.start(rim_s.at[0], rim_r.at[0], before)
    rim_lo = copies.start(rim_s.at[1], rim_r.at[1], after)
    for o, n in zip(ring, ar_in):
        copies.arrived(n, ar_z.at[around(16 - o)])
    total = jnp.zeros((1, ROW), f32)
    for a in range(0, 16, 4):
        total = total + ((ar_z[a] + ar_z[a + 1]) + (ar_z[a + 2] + ar_z[a + 3]))
    ar_p[x, y] = total
    plane = [(a, b) for a in range(4) for b in range(4) if a or b]
    ar_in = [
        copies.start(ar_p.at[x, y], ar_p.at[x, y], at_xy(a, b)) for a, b in plane
    ]
    copies.arrived(rim_hi, rim_r.at[0])
    copies.arrived(rim_lo, rim_r.at[1])
    for t in range(KW):
        zall[t, 7:8, :] = rim_r[1, t : t + 1, :]
        zall[t, 8 + TOK : 9 + TOK, :] = rim_r[0, t : t + 1, :]
    dyt[7:8, :] = rim_r[1, KW : KW + 1, :]
    dyt[8 + TOK : 9 + TOK, :] = rim_r[0, KW : KW + 1, :]

    @pl.loop(0, 4)
    def _(b):
        cols = pl.ds(pl.multiple_of(b * 256, 256), 256)

        def exact(mat, val):
            top = val.astype(bf16)
            low = (val - top.astype(f32)).astype(bf16)
            return dot(mat, top, NN) + dot(mat, low, NN)

        dhb[:, cols] = exact(three[...], zall[:, :, cols].reshape(KW * 64, 256))
        dyb[:, cols] = exact(one[...], dyt[:, cols])

    @pl.loop(0, ROWS // 16)
    def _(i):
        at = pl.ds(pl.multiple_of(i * 16, 16), 16)
        n = nbuf[at, :]
        dn = dhb[at, :] * dbuf[at, :]
        mid = jnp.mean(dn * n, axis=1, keepdims=True)
        r = rbuf[at, :][:, 0:1]
        dfeats[at, :] = (r * (dn - n * mid) + dyb[at, :]).astype(bf16)

    for o, n in zip(offs, dq_in):
        copies.arrived(n, dq_r.at[turn(zl, 4 - o)])
    for h in range(HEADS):
        dquery[:, h * QK : (h + 1) * QK] = dq_r[h]
    for o, n in zip(offs, kvg_in):
        copies.arrived(n, kvg_r.at[turn(zl, 4 - o)])
    for h in range(HEADS):
        dkey[:, h * QK : (h + 1) * QK] = kvg_r[h, :, 0:QK]
    for h in (0, 2):
        even = kvg_r[h, :, QK:].astype(f32)
        odd = pltpu.roll(kvg_r[h + 1, :, QK:].astype(f32), VD, 1)
        start = h * VD
        dvalue[:, start : start + VP] = jnp.where(lane < VD, even, odd).astype(bf16)
        dvalue[:, start + VP : start + VP + 128] = odd[:, 0:128].astype(bf16)

    for (a, b), n in zip(plane, ar_in):
        copies.arrived(n, ar_p.at[turn(x, 4 - a), turn(y, 4 - b)])
    total = jnp.zeros((1, ROW), f32)
    for a in range(4):
        total = total + ((ar_p[a, 0] + ar_p[a, 1]) + (ar_p[a, 2] + ar_p[a, 3]))
    dgain[...] = total[:, 0:C]
    loss_out[...] = total[:, C:]
    copies.finish()


def store_kernel(*refs):
    sems = refs[12]
    puts = [pltpu.make_async_copy(refs[i], refs[6 + i], sems.at[i]) for i in range(6)]
    for put in puts:
        put.start()
    for put in puts:
        put.wait()


def body(
    features,
    shift_offsets,
    conv_weight,
    norm_gain,
    query_proj,
    key_proj,
    value_proj,
    head_weight,
    targets,
    track_mask,
    track_pairing,
):
    wt = jnp.swapaxes(conv_weight, 1, 2).reshape(KW, 2, 16, C)
    vmem = pl.BlockSpec(memory_space=pltpu.VMEM)
    hbm = pl.BlockSpec(memory_space=pltpu.HBM)
    V = pltpu.VMEM
    scratch = [
        V((1, PAIRS), jnp.int32),
        V((1, C), f32),
        V((TOK, HEADS * VD), bf16),
        V((TOK, TRACKS), f32),
        V((PAIRS, TRACKS), jnp.int32),
        V((1, TRACKS), jnp.int32),
        V((KW, 4, 2, 2, 16, C), bf16),
        V((ROWS + 2 * RIM, C), bf16),
        V((ROWS + 2 * RIM, C), bf16),
        V((ROWS + 2 * RIM, C), bf16),
        V((ROWS + 2 * RIM, C), bf16),
        V((ROWS, C), f32),
        V((ROWS, C), f32),
        V((ROWS, 128), f32),
        V((C + HEADS * VD + VP - VD, TRACKS), bf16),
        V((4, 256, TRACKS), bf16),
        V((4, TOK, 512), bf16),
        V((4, 4, TOK, 512), bf16),
        V((4, TOK, VP), bf16),
        V((4, TOK, VP), bf16),
        V((4 * TOK, 16 * TOK), f32),
        V((4 * TOK, 16 * TOK), bf16),
        V((4, KW * TOK, C), bf16),
        V((4, KW * TOK, C), bf16),
        V((4, TOK, 256), bf16),
        V((4, TOK, 256), bf16),
        V((4, TOK, 256), bf16),
        V((4, TOK, 256), bf16),
        V((4, KW * TOK, C), bf16),
        V((4, KW * TOK, C), bf16),
        V((TOK, TRACKS), f32),
        V((TOK, TRACKS), bf16),
        V((TOK, TRACKS), bf16),
        V((TOK, TRACKS), bf16),
        V((TOK, TRACKS), bf16),
        V((TRACKS, TRACKS), bf16),
        V((TOK, TRACKS), f32),
        V((ROWS, KW * 64), bf16),
        V((ROWS, 64), bf16),
        V((4, TOK, VP), bf16),
        V((4, TOK, VP), bf16),
        V((4, TOK, QK), bf16),
        V((4, TOK, QK), bf16),
        V((4, 4, TOK, 384), bf16),
        V((4, 4, TOK, 384), bf16),
        V((4, TOK, 384), bf16),
        V((4, TOK, 384), bf16),
        V((64, C), f32),
        V((KW, 64, C), f32),
        V((2, 8, C), f32),
        V((2, 8, C), f32),
        V((ROWS, C), f32),
        V((ROWS, C), f32),
        V((1, C), f32),
        V((2, 1, ROW), f32),
        V((4, 4, 1, ROW), f32),
        V((16, 1, ROW), f32),
        pltpu.SemaphoreType.DMA((COPIES,)),
        pltpu.SemaphoreType.DMA((COPIES,)),
        pltpu.SemaphoreType.DMA((36,)),
    ]
    out = jax.ShapeDtypeStruct
    outs = pl.pallas_call(
        step_kernel,
        name="strand_step",
        out_shape=(
            out((ROWS, C), bf16),
            out((TOK, HEADS * QK), bf16),
            out((TOK, HEADS * QK), bf16),
            out((TOK, HEADS * VD), bf16),
            out((1, C), f32),
            out((1, 128), f32),
        ),
        in_specs=[hbm] * 11,
        out_specs=(vmem,) * 6,
        scratch_shapes=scratch,
        compiler_params=pltpu.CompilerParams(
            collective_id=0, has_side_effects=True, vmem_limit_bytes=48 << 20
        ),
    )(
        *(
            pltpu.with_memory_space_constraint(a, pltpu.HBM)
            for a in (
                features[0],
                shift_offsets.reshape(1, PAIRS),
                wt,
                norm_gain.reshape(1, C),
                query_proj[0],
                key_proj[0],
                value_proj[0],
                head_weight,
                targets[0],
                track_mask,
                track_pairing.reshape(1, TRACKS),
            )
        )
    )
    outs = pl.pallas_call(
        store_kernel,
        name="store",
        out_shape=tuple(out(o.shape, o.dtype) for o in outs),
        in_specs=[vmem] * 6,
        out_specs=(hbm,) * 6,
        scratch_shapes=[pltpu.SemaphoreType.DMA((6,))],
        compiler_params=pltpu.CompilerParams(vmem_limit_bytes=4 << 20),
    )(*outs)
    features_grad, query_grad, key_grad, value_grad, gain_grad, loss = outs
    return (
        features_grad[None],
        query_grad[None],
        key_grad[None],
        value_grad[None],
        gain_grad.reshape(C),
        loss[0, 0],
    )


def solution(mesh):
    placed = (
        P("dp", "seq", None),
        P(),
        P(None, None, "dp"),
        P(),
        P("dp", "seq", None),
        P("dp", "seq", None),
        P("dp", "seq", None),
        P(),
        P("dp", "seq", None),
        P(),
        P(),
    )
    return jax.shard_map(
        body,
        mesh=mesh,
        in_specs=placed,
        out_specs=(
            P("dp", "seq", None),
            P("dp", "seq", None),
            P("dp", "seq", None),
            P("dp", "seq", None),
            P(),
            P(),
        ),
        check_vma=False,
    )
```

```python
import math

import jax
import jax.numpy as jnp
from jax import lax
from jax.experimental import pallas as pl
from jax.experimental.pallas import tpu as pltpu
from jax.sharding import PartitionSpec as P

KW = 3
SHIFT = 4
POOL = 8
HEADS = 4
QK = 128
VD = 192
C = 1024
TRACKS = 512
ROWS = 256
TOK = 32
L16 = 4096
PAIRS = 16
RIM = 16
VP = 256
ROW = 1152
NORM_EPS = 1e-06
LOSS_SCALE = 1024.0
ROOT = math.sqrt(2.0 / math.pi)
CUBIC = 0.044715
COPIES = 126
f32 = jnp.float32
bf16 = jnp.bfloat16

NT = (((1,), (1,)), ((), ()))
NN = (((1,), (0,)), ((), ()))
TN = (((0,), (0,)), ((), ()))


def dot(a, b, dims):
    return lax.dot_general(a, b, dims, preferred_element_type=f32)


def iota(shape, axis):
    return lax.broadcasted_iota(jnp.int32, shape, axis)


class Copies:
    def __init__(self, send, recv):
        self.send, self.recv, self.used, self.sent = send, recv, 0, []

    def start(self, src, dst, device):
        n = self.used
        self.used += 1
        copy = pltpu.make_async_remote_copy(
            src_ref=src,
            dst_ref=dst,
            send_sem=self.send.at[n],
            recv_sem=self.recv.at[n],
            device_id=device,
            device_id_type=pl.DeviceIdType.MESH,
        )
        copy.start()
        self.sent.append(copy)
        return n

    def arrived(self, n, dst):
        pltpu.make_async_remote_copy(
            src_ref=dst,
            dst_ref=dst,
            send_sem=self.send.at[n],
            recv_sem=self.recv.at[n],
            device_id=self.someone,
            device_id_type=pl.DeviceIdType.MESH,
        ).wait_recv()

    def finish(self):
        assert self.used <= COPIES
        for copy in self.sent:
            copy.wait_send()


class Gather:
    def __init__(self, copies, device, unit):
        self.copies, self.device, self.unit = copies, device, unit

    def begin(self):
        mine = self.unit(0, None)
        self.right = self.copies.start(mine, mine, self.device(1))
        self.left = self.copies.start(mine, mine, self.device(3))

    def relay_from_left(self):
        self.copies.arrived(self.right, self.unit(3, None))
        part = self.unit(3, 0)
        self.far_right = self.copies.start(part, part, self.device(1))

    def relay_from_right(self):
        self.copies.arrived(self.left, self.unit(1, None))
        part = self.unit(1, 1)
        self.far_left = self.copies.start(part, part, self.device(3))

    def relay(self):
        self.relay_from_left()
        self.relay_from_right()

    def end(self):
        self.copies.arrived(self.far_right, self.unit(2, 0))
        self.copies.arrived(self.far_left, self.unit(2, 1))


class Direct(Gather):
    def begin(self):
        mine = self.unit(0, None)
        self.ins = [(o, self.copies.start(mine, mine, self.device(o))) for o in (1, 3, 2)]

    def end(self):
        for o, n in self.ins:
            self.copies.arrived(n, self.unit(4 - o, None))


def step_kernel(
    feats_in,
    offsets_in,
    wt_in,
    gain_in,
    query_in,
    key_in,
    value_in,
    head_in,
    targets_in,
    mask_in,
    pairing_in,
    dfeats,
    dquery,
    dkey,
    dvalue,
    dgain,
    loss_out,
    offsets,
    gain,
    value,
    targets,
    track_mask,
    pairing,
    wf,
    fext,
    hext,
    dnh,
    dnl,
    nbuf,
    dbuf,
    rbuf,
    head,
    headp,
    qkv,
    kva,
    att_s,
    att_r,
    probs,
    probs_b,
    taps,
    weigh,
    cv_s,
    cv_r,
    dyp_s,
    dyp_r,
    zp_s,
    zp_r,
    pre,
    pred_s,
    pred_r,
    tgt_s,
    tgt_r,
    pick,
    tgt_p,
    three,
    one,
    datt_s,
    datt_r,
    dq_s,
    dq_r,
    kvp_s,
    kvp_r,
    kvg_s,
    kvg_r,
    dyt,
    zall,
    rim_s,
    rim_r,
    edge_s,
    edge_r,
    edges,
    zr_f,
    zr_s,
    zr_r,
    dhb,
    dyb,
    gacc,
    ar_c,
    ar_p,
    ar_z,
    send_sem,
    recv_sem,
    own_sem,
):
    dp = lax.axis_index("dp")
    s = lax.axis_index("seq")
    zh, y, c = lax.div(dp, 8), lax.rem(lax.div(dp, 2), 4), lax.rem(dp, 2)
    x, zl = lax.div(s, 4), lax.rem(s, 4)

    def turn(a, o):
        return lax.rem(a + o, 4)

    def at_y(o):
        return {"dp": zh * 8 + turn(y, o) * 2 + c, "seq": s}

    def at_zh(o):
        return {"dp": turn(zh, o) * 8 + y * 2 + c, "seq": s}

    def at_x(o):
        return {"dp": dp, "seq": turn(x, o) * 4 + zl}

    def at_zl(o):
        return {"dp": dp, "seq": x * 4 + turn(zl, o)}

    other = {"dp": zh * 8 + y * 2 + (1 - c), "seq": s}
    after = {"dp": dp, "seq": lax.rem(s + 1, 16)}
    before = {"dp": dp, "seq": lax.rem(s + 15, 16)}

    barrier = pltpu.get_barrier_semaphore()
    peers = [f(o) for f in (at_x, at_zl) for o in (1, 2, 3)]
    peers += [f(o) for f in (at_y, at_zh) for o in (1, 3)]
    peers += [other, after, before]
    offs = (1, 2, 3)

    def at_xy(a, b):
        return {"dp": zh * 8 + turn(y, b) * 2 + c, "seq": turn(x, a) * 4 + zl}


    def around(o):
        return lax.rem(zh * 4 + zl + o, 16)

    def at_z(o):
        z = around(o)
        return {"dp": lax.div(z, 4) * 8 + y * 2 + c, "seq": x * 4 + lax.rem(z, 4)}
    for peer in peers:
        pl.semaphore_signal(
            barrier, inc=1, device_id=peer, device_id_type=pl.DeviceIdType.MESH
        )
    copies = Copies(send_sem, recv_sem)
    copies.someone = other

    pulls = []

    def pull(src, dst):
        pulls.append(pltpu.make_async_copy(src, dst, own_sem.at[len(pulls)]))
        pulls[-1].start()
        return pulls[-1]

    wt_pull = pull(wt_in, wf.at[:, 0, c])
    qkv_pulls = [pull(value_in, value)]
    for h in range(HEADS):
        cols = pl.ds(h * QK, QK)
        qkv_pulls.append(pull(query_in.at[:, cols], qkv.at[h, :, pl.ds(0, QK)]))
        qkv_pulls.append(pull(key_in.at[:, cols], qkv.at[h, :, pl.ds(QK, QK)]))
    feats_pulls = [pull(gain_in, gain), pull(feats_in, fext.at[pl.ds(RIM, ROWS)])]
    rest_pulls = [
        pull(targets_in, targets),
        pull(offsets_in, offsets),
        pull(mask_in, track_mask),
        pull(pairing_in, pairing),
    ]
    rows = C + HEADS * VD
    head_copies = [pull(head_in, head.at[pl.ds(0, rows)])]
    for a in range(4):
        for b in range(4):
            start = pl.multiple_of(256 * turn(zh, b) + 64 * a, 64)
            block = head_in.at[pl.ds(start, 64)]
            head_copies.append(pull(block, headp.at[a, pl.ds(64 * b, 64)]))
    fext[0:8, :] = jnp.zeros((8, C), bf16)
    fext[2 * RIM + ROWS - 8 :, :] = jnp.zeros((8, C), bf16)
    head[rows:, :] = jnp.zeros((VP - VD, TRACKS), bf16)

    def columns(o, half):
        if half is None:
            return pl.ds(pl.multiple_of(turn(x, o) * 256, 128), 256)
        return pl.ds(pl.multiple_of(turn(x, o) * 256 + 128 * half, 128), 128)

    def slot(t, r, half):
        if half is None:
            return wf.at[t, r, c, :, :, columns(0, None)]
        return wf.at[t, r, c, half, :, columns(0, None)]

    def unit_yx(t, r):
        return lambda o, half: wf.at[t, r, c, :, :, columns(o, half)]

    def unit_of(buf):
        def unit(o, half):
            if half is None:
                return buf.at[turn(y, o)]
            return buf.at[turn(y, o), pl.ds(half * 48, 48), :]

        return unit

    kv_cols = pl.ds(QK, 3 * QK)

    def unit_kv(o, half):
        if half is None:
            return kva.at[turn(x, o), :, :, kv_cols]
        return kva.at[turn(x, o), pl.ds(2 * half, 2), :, kv_cols]

    g_yx = [[Direct(copies, at_x, unit_yx(t, r)) for r in range(4)] for t in range(KW)]
    g_taps = Gather(copies, at_y, unit_of(taps))
    g_weigh = Gather(copies, at_y, unit_of(weigh))
    g_kv = Direct(copies, at_x, unit_kv)
    wt_pull.wait()
    pl.semaphore_wait(barrier, len(peers))
    for pulled in feats_pulls:
        pulled.wait()
    edge = pl.ds(RIM + ROWS, 8)
    lo = copies.start(fext.at[pl.ds(ROWS + 8, 8)], fext.at[pl.ds(8, 8)], after)
    hi = copies.start(fext.at[pl.ds(RIM, 8)], fext.at[edge], before)
    z_in = []
    for t in range(KW):
        right = copies.start(slot(t, 0, None), slot(t, 3, None), at_zh(1))
        left = copies.start(slot(t, 0, None), slot(t, 1, None), at_zh(3))
        z_in.append((right, left))
    pair_in = []

    def share(r, t=None):
        taps_of = pl.ds(0, KW) if t is None else t
        part = wf.at[taps_of, r, c]
        n = copies.start(part, part, other)
        pair_in.append((r, n, wf.at[taps_of, r, 1 - c]))

    share(0)

    for pulled in qkv_pulls:
        pulled.wait()
    lane = iota((TOK, VP), 1)
    vals = value[...].astype(f32)
    for h in range(HEADS):
        start = h * VD
        if h % 2 == 0:
            cut = vals[:, start : start + VP]
        else:
            cut = pltpu.roll(vals[:, start - 64 : start + VD], VP - 64, 1)
        qkv[h, :, 2 * QK :] = jnp.where(lane < VD, cut, 0.0).astype(bf16)
    kva[x, zl] = qkv[zl]
    qkv_in = [
        copies.start(qkv.at[turn(zl, o)], kva.at[x, zl], at_zl(o)) for o in offs
    ]
    def normed(row):
        f = fext[pl.ds(row, 16), :].astype(f32)
        r = lax.rsqrt(jnp.mean(f * f, axis=1, keepdims=True) + NORM_EPS)
        n = f * r
        g = n * gain[...]
        sq = g * g
        t = jnp.tanh(ROOT * (g + CUBIC * (sq * g)))
        return n, g, sq, t, r

    def hidden(row):
        n, g, sq, t, r = normed(row)
        hext[pl.ds(row, 16), :] = (0.5 * g * (1.0 + t)).astype(bf16)

    def slopes(row):
        n, g, sq, t, r = normed(row)
        slope = 0.5 * (1.0 + t) + (0.5 * ROOT) * g * (1.0 - t * t) * (
            1.0 + (3.0 * CUBIC) * sq
        )
        dn = slope * n
        top = dn.astype(bf16)
        dnh[pl.ds(row, 16), :] = top
        dnl[pl.ds(row, 16), :] = (dn - top.astype(f32)).astype(bf16)
        return n, slope, r

    @pl.loop(1, 1 + ROWS // 16)
    def _(i):
        hidden(pl.multiple_of(i * 16, 16))

    for pulled in rest_pulls:
        pulled.wait()
    flip = dp >= PAIRS
    interval = lax.rem(dp, PAIRS)
    sign = jnp.where(flip, -1, 1)
    mine = iota((1, PAIRS), 1) == interval
    chosen = jnp.sum(jnp.where(mine, offsets[...].astype(f32), 0.0), axis=1, keepdims=True)
    off = chosen.astype(jnp.int32) * sign

    EXT = ROWS + 2 * RIM

    def mean_matrix(count, shift_of):
        row, col = iota((count, EXT), 0), iota((count, EXT), 1)
        tok = lax.rem(row, TOK)
        at = col - RIM
        rel = at + off - shift_of(row) - POOL * tok
        where_p = s * ROWS + at + off
        where_q = s * ROWS + at
        fine = (rel >= 0) & (rel < POOL) & (where_p >= 0) & (where_p < L16)
        fine = fine & (where_q >= 0) & (where_q < L16)
        return jnp.where(fine, 1.0 / POOL, 0.0).astype(bf16)

    mix = mean_matrix(KW * TOK, lambda row: (lax.div(row, TOK) - 1) * sign)
    still = mean_matrix(TOK, lambda row: 0 * row)
    copies.arrived(lo, fext.at[pl.ds(8, 8)])
    copies.arrived(hi, fext.at[edge])
    hidden(0)
    hidden(RIM + ROWS)
    taps[y] = dot(mix, hext[...], NN).astype(bf16)
    g_taps.begin()
    pooled_u = dot(still, fext[...], NN).astype(bf16)

    def later(first, last):
        @pl.loop(first, last)
        def _(i):
            row = pl.multiple_of(i * 16, 16)
            n, slope, r = slopes(pl.multiple_of(row + RIM, 16))
            nbuf[pl.ds(row, 16), :] = n
            dbuf[pl.ds(row, 16), :] = slope * gain[...]
            rbuf[pl.ds(row, 16), :] = jnp.broadcast_to(r, (16, 128))

    z_far = []
    for t in range(KW):
        right, left = z_in[t]
        copies.arrived(right, slot(t, 3, None))
        to_right = copies.start(slot(t, 3, 0), slot(t, 2, 0), at_zh(1))
        g_yx[t][3].begin()
        copies.arrived(left, slot(t, 1, None))
        to_left = copies.start(slot(t, 1, 1), slot(t, 2, 1), at_zh(3))
        g_yx[t][1].begin()
        z_far.append((to_right, to_left))
    for o, n in zip(offs, qkv_in):
        copies.arrived(n, kva.at[x, turn(zl, 4 - o)])
    g_kv.begin()
    g_taps.relay()
    for pulled in head_copies:
        pulled.wait()
    pre[...] = dot(pooled_u, head[0:C, :], NN)
    def spread(width, tap_of):
        row, col = iota((ROWS, width), 0), iota((ROWS, width), 1)
        reach = row + off - tap_of(col)
        at = s * ROWS + row + off
        seen = s * ROWS + reach
        fine = (lax.shift_right_arithmetic(reach + 64, 3) == lax.rem(col, 64)) & (at >= 0)
        fine = fine & (at < L16) & (seen >= 0) & (seen < L16)
        return jnp.where(fine, 1.0, 0.0).astype(bf16)

    three[...] = spread(192, lambda col: (lax.div(col, 64) - 1) * sign)
    one[...] = spread(64, lambda col: 0 * col)
    dyt[...] = jnp.zeros((64, C), f32)
    zall[...] = jnp.zeros((KW, 64, C), f32)
    edges[...] = jnp.zeros((16, 256), f32)
    zr_f[...] = jnp.zeros((4, 8, C), f32)

    later(0, 8)
    for t in range(KW):
        to_right, to_left = z_far[t]
        copies.arrived(to_right, slot(t, 2, 0))
        copies.arrived(to_left, slot(t, 2, 1))
        g_yx[t][2].begin()
    tgt_s[...] = targets[...].astype(bf16)
    tgt_in = copies.start(tgt_s, tgt_r, at_zh(2))
    for r in (3, 1):
        for t in range(KW):
            g_yx[t][r].end()
        share(r)
    g_taps.end()

    def convolve(r):
        for q, n, part in pair_in:
            if q == r:
                copies.arrived(n, part)
        acc = jnp.zeros((4 * TOK, 64), f32)
        for t in range(KW):
            rows_t = taps[:, t * TOK : (t + 1) * TOK, :].reshape(4 * TOK, C)
            acc = acc + dot(rows_t, wf[t, r].reshape(64, C), NT)
        cv_s[:, :, r * 64 : (r + 1) * 64] = acc.astype(bf16).reshape(4, TOK, 64)

    convolve(0)
    g_kv.end()
    inv_sqrt = 1.0 / math.sqrt(QK)
    qh = kva[x, :, :, 0:QK].reshape(4 * TOK, QK)
    kh = kva[:, :, :, QK : 2 * QK].reshape(16 * TOK, QK)
    vh = kva[:, :, :, 2 * QK :].reshape(16 * TOK, VP)
    scores = dot(qh, kh, NT) * inv_sqrt
    e = jnp.exp(scores - jnp.max(scores, axis=1, keepdims=True))
    p = e / jnp.sum(e, axis=1, keepdims=True)
    probs[...] = p
    probs_b[...] = p.astype(bf16)
    att_s[...] = dot(probs_b[...], vh, NN).astype(bf16).reshape(4, TOK, VP)
    att_r[zl] = att_s[zl]
    att_in = [
        copies.start(att_s.at[turn(zl, o)], att_r.at[zl], at_zl(o)) for o in offs
    ]
    for t in range(KW):
        g_yx[t][2].end()
        share(2, t)
    convolve(3)
    convolve(1)
    convolve(2)
    cv_r[y] = cv_s[y]
    cv_in = [copies.start(cv_s.at[turn(y, o)], cv_r.at[y], at_y(o)) for o in offs]
    slopes(0)
    slopes(RIM + ROWS)
    later(8, 16)
    both = dot(mix, dnh[...], NN) + dot(mix, dnl[...], NN)
    weigh[y] = (both * POOL).astype(bf16)
    g_weigh.begin()
    pick[...] = jnp.where(
        iota((TRACKS, TRACKS), 0) == pairing[...], 1.0, 0.0
    ).astype(bf16)
    mrow = track_mask[pl.ds(interval, 1), :].astype(f32)
    count = jnp.maximum(jnp.sum(mrow, axis=1, keepdims=True), 1.0)
    mpair = dot(jnp.broadcast_to(mrow, (16, TRACKS)).astype(bf16), pick[...], NN)[0:1, :]
    for o, n in zip(offs, att_in):
        copies.arrived(n, att_r.at[turn(zl, 4 - o)])
    for h in range(HEADS):
        pre[...] += dot(att_r[h], head[C + h * VD : C + h * VD + VP, :], NN)
    for o, n in zip(offs, cv_in):
        copies.arrived(n, cv_r.at[turn(y, 4 - o)])

    logits = pre[...]
    for a in range(4):
        logits = logits + dot(cv_r[a], headp[a], NN)
    pred = jnp.maximum(logits, 0.0) + jnp.log1p(jnp.exp(-jnp.abs(logits)))
    pred_s[...] = pred.astype(bf16)
    pred_in = copies.start(pred_s, pred_r, at_zh(2))
    gate = jax.nn.sigmoid(logits)
    copies.arrived(tgt_in, tgt_r)
    tgt_p[...] = dot(tgt_r[...], pick[...], NN)
    g_weigh.relay()
    copies.arrived(pred_in, pred_r)
    both = 0.5 * (pred + dot(pred_r[...], pick[...], NN))
    misfit = both - targets[...]
    weighted = mrow * misfit
    dpred = (LOSS_SCALE / count) * (weighted + mpair * (both - tgt_p[...]))
    dlogit = (dpred * gate).astype(bf16)

    for a in range(4):
        part = dot(dlogit, headp[a], NT) * (1.0 / POOL)
        dyp_s[a] = part.astype(bf16)
    dyp_r[y] = dyp_s[y]
    dyp_in = [copies.start(dyp_s.at[turn(y, o)], dyp_r.at[y], at_y(o)) for o in offs]
    for h in range(HEADS):
        part = dot(dlogit, head[C + h * VD : C + h * VD + VP, :], NT)
        datt_s[h] = jnp.where(lane < VD, part, 0.0).astype(bf16)
    datt_r[zl] = datt_s[zl]
    datt_in = [
        copies.start(datt_s.at[turn(zl, o)], datt_r.at[zl], at_zl(o)) for o in offs
    ]
    dyt[8 : 8 + TOK, :] = dot(dlogit, head[0:C, :], NT) * (1.0 / POOL)
    rim_s[0] = dyt[8:9, :]
    rim_s[1] = dyt[7 + TOK : 8 + TOK, :]
    rim_hi = copies.start(rim_s.at[0], rim_r.at[0], before)
    rim_lo = copies.start(rim_s.at[1], rim_r.at[1], after)

    loss = jnp.sum(jnp.sum(weighted * misfit, axis=1, keepdims=True), axis=0, keepdims=True)
    loss = loss / count / (2.0 * PAIRS * TOK * 16)
    g_weigh.end()
    for o, n in zip(offs, dyp_in):
        copies.arrived(n, dyp_r.at[turn(y, 4 - o)])
    for a in range(4):
        cols = slice(a * 256, (a + 1) * 256)
        edge_s[0, :, cols] = dyp_r[a, 0:1, :].astype(f32)
        edge_s[1, :, cols] = dyp_r[a, TOK - 1 : TOK, :].astype(f32)
    edge_hi = copies.start(edge_s.at[0], edge_r.at[0], before)
    edge_lo = copies.start(edge_s.at[1], edge_r.at[1], after)
    @pl.loop(0, 4)
    def _(b):
        cols = pl.ds(pl.multiple_of(b * 256, 256), 256)
        gains = jnp.zeros((4 * TOK, 256), f32)
        dyr = dyp_r[...].reshape(4 * TOK, 256)
        for t in range(KW):
            part = pl.ds(t * TOK, TOK)
            w = wf[t, :, :, :, :, cols].reshape(256, 256)
            acc = dot(dyr, w, NN)
            zp_s[:, part, cols] = acc.astype(bf16).reshape(4, TOK, 256)
            gains = gains + acc * weigh[:, part, cols].reshape(4 * TOK, 256).astype(f32)
        gacc[:, cols] = jnp.sum(gains, axis=0, keepdims=True)

    zp_in = [copies.start(zp_s.at[turn(y, o)], zp_r.at[y], at_y(o)) for o in offs]
    zp_r[y] = zp_s[y]

    ar_c[c] = jnp.concatenate([gacc[...], jnp.broadcast_to(loss, (1, 128))], axis=1)
    ar_in = copies.start(ar_c.at[c], ar_c.at[c], other)
    for o, n in zip(offs, datt_in):
        copies.arrived(n, datt_r.at[turn(zl, 4 - o)])
    dout = datt_r[...].reshape(4 * TOK, VP)
    att = att_s[...].reshape(4 * TOK, VP)
    delta = jnp.sum(dout.astype(f32) * att.astype(f32), axis=1, keepdims=True)
    vh = kva[:, :, :, 2 * QK :].reshape(16 * TOK, VP)
    ds = (probs[...] * (dot(dout, vh, NT) - delta)).astype(bf16)
    qh = kva[x, :, :, 0:QK].reshape(4 * TOK, QK)
    kvp_s[:, :, :, 0:QK] = dot(ds, qh, TN).astype(bf16).reshape(4, 4, TOK, QK)
    kvp_s[:, :, :, QK:] = dot(probs_b[...], dout, TN).astype(bf16).reshape(4, 4, TOK, VP)
    kvp_in = [copies.start(kvp_s.at[turn(x, o)], kvp_r.at[x], at_x(o)) for o in offs]
    kh = kva[:, :, :, QK : 2 * QK].reshape(16 * TOK, QK)
    dq_s[...] = (dot(ds, kh, NN) * inv_sqrt).astype(bf16).reshape(4, TOK, QK)
    dq_r[zl] = dq_s[zl]
    dq_in = [copies.start(dq_s.at[turn(zl, o)], dq_r.at[zl], at_zl(o)) for o in offs]
    copies.arrived(ar_in, ar_c.at[1 - c])
    ar_z[around(0)] = ar_c[0] + ar_c[1]
    ring = (8, 7, 9, 6, 10, 5, 11, 4, 12, 3, 13, 2, 14, 1, 15)
    ar_in = [copies.start(ar_z.at[around(0)], ar_z.at[around(0)], at_z(o)) for o in ring]

    copies.arrived(edge_hi, edge_r.at[0])
    copies.arrived(edge_lo, edge_r.at[1])
    for a in range(4):
        cols = slice(a * 256, (a + 1) * 256)
        edges[a : a + 1, :] = edge_r[0][:, cols]
        edges[8 + a : 9 + a, :] = edge_r[1][:, cols]
    both = edges[...].astype(bf16)
    for t in range(KW):
        res = dot(both, wf[t].reshape(256, C), NN)
        for a in range(4):
            zr_f[a, t : t + 1, :] = res[a : a + 1, :]
            zr_f[a, KW + t : KW + t + 1, :] = res[8 + a : 9 + a, :]
    zr_s[...] = zr_f[...].astype(bf16)
    zr_r[y] = zr_s[y]
    zr_in = [copies.start(zr_s.at[turn(y, o)], zr_r.at[y], at_y(o)) for o in offs]
    for o, n in zip(offs, kvp_in):
        copies.arrived(n, kvp_r.at[turn(x, 4 - o)])
    total = kvp_s[x].astype(f32)
    for o in offs:
        total = total + kvp_r[turn(x, o)].astype(f32)
    kvg_s[:, :, 0:QK] = (total[:, :, 0:QK] * inv_sqrt).astype(bf16)
    kvg_s[:, :, QK:] = total[:, :, QK:].astype(bf16)
    kvg_r[zl] = kvg_s[zl]
    kvg_in = [
        copies.start(kvg_s.at[turn(zl, o)], kvg_r.at[zl], at_zl(o)) for o in offs
    ]
    for o, n in zip(ring, ar_in):
        copies.arrived(n, ar_z.at[around(16 - o)])
    total = jnp.zeros((1, ROW), f32)
    for a in range(0, 16, 4):
        total = total + ((ar_z[a] + ar_z[a + 1]) + (ar_z[a + 2] + ar_z[a + 3]))
    ar_p[x, y] = total
    plane = [(a, b) for a in range(4) for b in range(4) if a or b]
    ar_in = [
        copies.start(ar_p.at[x, y], ar_p.at[x, y], at_xy(a, b)) for a, b in plane
    ]
    for o, n in zip(offs, zp_in):
        copies.arrived(n, zp_r.at[turn(y, 4 - o)])

    @pl.loop(0, 4)
    def _(b):
        cols = pl.ds(pl.multiple_of(b * 256, 256), 256)
        for t in range(KW):
            part = pl.ds(t * TOK, TOK)
            low = zp_r[0, part, cols].astype(f32) + zp_r[1, part, cols].astype(f32)
            high = zp_r[2, part, cols].astype(f32) + zp_r[3, part, cols].astype(f32)
            zall[t, 8 : 8 + TOK, cols] = low + high

    copies.arrived(rim_hi, rim_r.at[0])
    copies.arrived(rim_lo, rim_r.at[1])
    for o, n in zip(offs, zr_in):
        copies.arrived(n, zr_r.at[turn(y, 4 - o)])
    low = zr_r[0].astype(f32) + zr_r[1].astype(f32)
    beside = low + (zr_r[2].astype(f32) + zr_r[3].astype(f32))
    for t in range(KW):
        zall[t, 8 + TOK : 9 + TOK, :] = beside[t : t + 1, :]
        zall[t, 7:8, :] = beside[KW + t : KW + t + 1, :]
    dyt[7:8, :] = rim_r[1]
    dyt[8 + TOK : 9 + TOK, :] = rim_r[0]

    @pl.loop(0, 4)
    def _(b):
        cols = pl.ds(pl.multiple_of(b * 256, 256), 256)

        def exact(mat, val):
            top = val.astype(bf16)
            low = (val - top.astype(f32)).astype(bf16)
            return dot(mat, top, NN) + dot(mat, low, NN)

        dhb[:, cols] = exact(three[...], zall[:, :, cols].reshape(KW * 64, 256))
        dyb[:, cols] = exact(one[...], dyt[:, cols])

    @pl.loop(0, ROWS // 16)
    def _(i):
        at = pl.ds(pl.multiple_of(i * 16, 16), 16)
        n = nbuf[at, :]
        dn = dhb[at, :] * dbuf[at, :]
        mid = jnp.mean(dn * n, axis=1, keepdims=True)
        r = rbuf[at, :][:, 0:1]
        dfeats[at, :] = (r * (dn - n * mid) + dyb[at, :]).astype(bf16)

    for o, n in zip(offs, dq_in):
        copies.arrived(n, dq_r.at[turn(zl, 4 - o)])
    for h in range(HEADS):
        dquery[:, h * QK : (h + 1) * QK] = dq_r[h]
    for o, n in zip(offs, kvg_in):
        copies.arrived(n, kvg_r.at[turn(zl, 4 - o)])
    for h in range(HEADS):
        dkey[:, h * QK : (h + 1) * QK] = kvg_r[h, :, 0:QK]
    for h in (0, 2):
        even = kvg_r[h, :, QK:].astype(f32)
        odd = pltpu.roll(kvg_r[h + 1, :, QK:].astype(f32), VD, 1)
        start = h * VD
        dvalue[:, start : start + VP] = jnp.where(lane < VD, even, odd).astype(bf16)
        dvalue[:, start + VP : start + VP + 128] = odd[:, 0:128].astype(bf16)

    for (a, b), n in zip(plane, ar_in):
        copies.arrived(n, ar_p.at[turn(x, 4 - a), turn(y, 4 - b)])
    total = jnp.zeros((1, ROW), f32)
    for a in range(4):
        total = total + ((ar_p[a, 0] + ar_p[a, 1]) + (ar_p[a, 2] + ar_p[a, 3]))
    dgain[...] = total[:, 0:C]
    loss_out[...] = total[:, C:]
    copies.finish()


def store_kernel(*refs):
    sems = refs[12]
    puts = [pltpu.make_async_copy(refs[i], refs[6 + i], sems.at[i]) for i in range(6)]
    for put in puts:
        put.start()
    for put in puts:
        put.wait()


def body(
    features,
    shift_offsets,
    conv_weight,
    norm_gain,
    query_proj,
    key_proj,
    value_proj,
    head_weight,
    targets,
    track_mask,
    track_pairing,
):
    wt = jnp.swapaxes(conv_weight, 1, 2).reshape(KW, 2, 16, C)
    vmem = pl.BlockSpec(memory_space=pltpu.VMEM)
    hbm = pl.BlockSpec(memory_space=pltpu.HBM)
    V = pltpu.VMEM
    scratch = [
        V((1, PAIRS), jnp.int32),
        V((1, C), f32),
        V((TOK, HEADS * VD), bf16),
        V((TOK, TRACKS), f32),
        V((PAIRS, TRACKS), jnp.int32),
        V((1, TRACKS), jnp.int32),
        V((KW, 4, 2, 2, 16, C), bf16),
        V((ROWS + 2 * RIM, C), bf16),
        V((ROWS + 2 * RIM, C), bf16),
        V((ROWS + 2 * RIM, C), bf16),
        V((ROWS + 2 * RIM, C), bf16),
        V((ROWS, C), f32),
        V((ROWS, C), f32),
        V((ROWS, 128), f32),
        V((C + HEADS * VD + VP - VD, TRACKS), bf16),
        V((4, 256, TRACKS), bf16),
        V((4, TOK, 512), bf16),
        V((4, 4, TOK, 512), bf16),
        V((4, TOK, VP), bf16),
        V((4, TOK, VP), bf16),
        V((4 * TOK, 16 * TOK), f32),
        V((4 * TOK, 16 * TOK), bf16),
        V((4, KW * TOK, C), bf16),
        V((4, KW * TOK, C), bf16),
        V((4, TOK, 256), bf16),
        V((4, TOK, 256), bf16),
        V((4, TOK, 256), bf16),
        V((4, TOK, 256), bf16),
        V((4, KW * TOK, C), bf16),
        V((4, KW * TOK, C), bf16),
        V((TOK, TRACKS), f32),
        V((TOK, TRACKS), bf16),
        V((TOK, TRACKS), bf16),
        V((TOK, TRACKS), bf16),
        V((TOK, TRACKS), bf16),
        V((TRACKS, TRACKS), bf16),
        V((TOK, TRACKS), f32),
        V((ROWS, KW * 64), bf16),
        V((ROWS, 64), bf16),
        V((4, TOK, VP), bf16),
        V((4, TOK, VP), bf16),
        V((4, TOK, QK), bf16),
        V((4, TOK, QK), bf16),
        V((4, 4, TOK, 384), bf16),
        V((4, 4, TOK, 384), bf16),
        V((4, TOK, 384), bf16),
        V((4, TOK, 384), bf16),
        V((64, C), f32),
        V((KW, 64, C), f32),
        V((2, 1, C), f32),
        V((2, 1, C), f32),
        V((2, 1, C), f32),
        V((2, 1, C), f32),
        V((16, 256), f32),
        V((4, 8, C), f32),
        V((4, 8, C), bf16),
        V((4, 8, C), bf16),
        V((ROWS, C), f32),
        V((ROWS, C), f32),
        V((1, C), f32),
        V((2, 1, ROW), f32),
        V((4, 4, 1, ROW), f32),
        V((16, 1, ROW), f32),
        pltpu.SemaphoreType.DMA((COPIES,)),
        pltpu.SemaphoreType.DMA((COPIES,)),
        pltpu.SemaphoreType.DMA((36,)),
    ]
    out = jax.ShapeDtypeStruct
    outs = pl.pallas_call(
        step_kernel,
        name="strand_step",
        out_shape=(
            out((ROWS, C), bf16),
            out((TOK, HEADS * QK), bf16),
            out((TOK, HEADS * QK), bf16),
            out((TOK, HEADS * VD), bf16),
            out((1, C), f32),
            out((1, 128), f32),
        ),
        in_specs=[hbm] * 11,
        out_specs=(vmem,) * 6,
        scratch_shapes=scratch,
        compiler_params=pltpu.CompilerParams(
            collective_id=0, has_side_effects=True, vmem_limit_bytes=48 << 20
        ),
    )(
        *(
            pltpu.with_memory_space_constraint(a, pltpu.HBM)
            for a in (
                features[0],
                shift_offsets.reshape(1, PAIRS),
                wt,
                norm_gain.reshape(1, C),
                query_proj[0],
                key_proj[0],
                value_proj[0],
                head_weight,
                targets[0],
                track_mask,
                track_pairing.reshape(1, TRACKS),
            )
        )
    )
    outs = pl.pallas_call(
        store_kernel,
        name="store",
        out_shape=tuple(out(o.shape, o.dtype) for o in outs),
        in_specs=[vmem] * 6,
        out_specs=(hbm,) * 6,
        scratch_shapes=[pltpu.SemaphoreType.DMA((6,))],
        compiler_params=pltpu.CompilerParams(vmem_limit_bytes=4 << 20),
    )(*outs)
    features_grad, query_grad, key_grad, value_grad, gain_grad, loss = outs
    return (
        features_grad[None],
        query_grad[None],
        key_grad[None],
        value_grad[None],
        gain_grad.reshape(C),
        loss[0, 0],
    )


def solution(mesh):
    placed = (
        P("dp", "seq", None),
        P(),
        P(None, None, "dp"),
        P(),
        P("dp", "seq", None),
        P("dp", "seq", None),
        P("dp", "seq", None),
        P(),
        P("dp", "seq", None),
        P(),
        P(),
    )
    return jax.shard_map(
        body,
        mesh=mesh,
        in_specs=placed,
        out_specs=(
            P("dp", "seq", None),
            P("dp", "seq", None),
            P("dp", "seq", None),
            P("dp", "seq", None),
            P(),
            P(),
        ),
        check_vma=False,
    )
```

```python
import math

import jax
import jax.numpy as jnp
from jax import lax
from jax.experimental import pallas as pl
from jax.experimental.pallas import tpu as pltpu
from jax.sharding import PartitionSpec as P

KW = 3
SHIFT = 4
POOL = 8
HEADS = 4
QK = 128
VD = 192
C = 1024
TRACKS = 512
ROWS = 256
TOK = 32
L16 = 4096
PAIRS = 16
RIM = 16
VP = 256
ROW = 1152
NORM_EPS = 1e-06
LOSS_SCALE = 1024.0
ROOT = math.sqrt(2.0 / math.pi)
CUBIC = 0.044715
COPIES = 142
f32 = jnp.float32
bf16 = jnp.bfloat16

NT = (((1,), (1,)), ((), ()))
NN = (((1,), (0,)), ((), ()))
TN = (((0,), (0,)), ((), ()))


def dot(a, b, dims):
    return lax.dot_general(a, b, dims, preferred_element_type=f32)


def iota(shape, axis):
    return lax.broadcasted_iota(jnp.int32, shape, axis)


class Copies:
    def __init__(self, send, recv):
        self.send, self.recv, self.used, self.sent = send, recv, 0, []

    def start(self, src, dst, device):
        n = self.used
        self.used += 1
        copy = pltpu.make_async_remote_copy(
            src_ref=src,
            dst_ref=dst,
            send_sem=self.send.at[n],
            recv_sem=self.recv.at[n],
            device_id=device,
            device_id_type=pl.DeviceIdType.MESH,
        )
        copy.start()
        self.sent.append(copy)
        return n

    def arrived(self, n, dst):
        pltpu.make_async_remote_copy(
            src_ref=dst,
            dst_ref=dst,
            send_sem=self.send.at[n],
            recv_sem=self.recv.at[n],
            device_id=self.someone,
            device_id_type=pl.DeviceIdType.MESH,
        ).wait_recv()

    def finish(self):
        assert self.used <= COPIES
        for copy in self.sent:
            copy.wait_send()


class Gather:
    def __init__(self, copies, device, unit):
        self.copies, self.device, self.unit = copies, device, unit

    def begin(self):
        mine = self.unit(0, None)
        self.right = self.copies.start(mine, mine, self.device(1))
        self.left = self.copies.start(mine, mine, self.device(3))

    def relay_from_left(self):
        self.copies.arrived(self.right, self.unit(3, None))
        part = self.unit(3, 0)
        self.far_right = self.copies.start(part, part, self.device(1))

    def relay_from_right(self):
        self.copies.arrived(self.left, self.unit(1, None))
        part = self.unit(1, 1)
        self.far_left = self.copies.start(part, part, self.device(3))

    def relay(self):
        self.relay_from_left()
        self.relay_from_right()

    def end(self):
        self.copies.arrived(self.far_right, self.unit(2, 0))
        self.copies.arrived(self.far_left, self.unit(2, 1))


class Direct(Gather):
    def begin(self):
        mine = self.unit(0, None)
        self.ins = [(o, self.copies.start(mine, mine, self.device(o))) for o in (1, 3, 2)]

    def end(self):
        for o, n in self.ins:
            self.copies.arrived(n, self.unit(4 - o, None))


def step_kernel(
    feats_in,
    offsets_in,
    wt_in,
    gain_in,
    query_in,
    key_in,
    value_in,
    head_in,
    targets_in,
    mask_in,
    pairing_in,
    dfeats,
    dquery,
    dkey,
    dvalue,
    dgain,
    loss_out,
    offsets,
    gain,
    value,
    targets,
    track_mask,
    pairing,
    wf,
    fext,
    hext,
    dnh,
    dnl,
    nbuf,
    dbuf,
    rbuf,
    head,
    headp,
    qkv,
    kva,
    att_s,
    att_r,
    probs,
    probs_b,
    taps,
    weigh,
    cv_s,
    cv_r,
    dyp_s,
    dyp_r,
    zp_s,
    zp_r,
    pre,
    pred_s,
    pred_r,
    tgt_s,
    tgt_r,
    pick,
    tgt_p,
    three,
    one,
    datt_s,
    datt_r,
    dq_s,
    dq_r,
    kvp_s,
    kvp_r,
    kvg_s,
    kvg_r,
    dyt,
    zall,
    rim_s,
    rim_r,
    edge_s,
    edge_r,
    edges,
    zr_f,
    zr_s,
    zr_r,
    dhb,
    dyb,
    gacc,
    ar_p,
    ar_z,
    send_sem,
    recv_sem,
    own_sem,
):
    dp = lax.axis_index("dp")
    s = lax.axis_index("seq")
    zh, y, c = lax.div(dp, 8), lax.rem(lax.div(dp, 2), 4), lax.rem(dp, 2)
    x, zl = lax.div(s, 4), lax.rem(s, 4)

    def turn(a, o):
        return lax.rem(a + o, 4)

    def at_y(o):
        return {"dp": zh * 8 + turn(y, o) * 2 + c, "seq": s}

    def at_zh(o):
        return {"dp": turn(zh, o) * 8 + y * 2 + c, "seq": s}

    def at_x(o):
        return {"dp": dp, "seq": turn(x, o) * 4 + zl}

    def at_zl(o):
        return {"dp": dp, "seq": x * 4 + turn(zl, o)}

    other = {"dp": zh * 8 + y * 2 + (1 - c), "seq": s}
    after = {"dp": dp, "seq": lax.rem(s + 1, 16)}
    before = {"dp": dp, "seq": lax.rem(s + 15, 16)}

    barrier = pltpu.get_barrier_semaphore()
    peers = [f(o) for f in (at_x, at_zl) for o in (1, 2, 3)]
    peers += [f(o) for f in (at_y, at_zh) for o in (1, 3)]
    peers += [other, after, before]
    offs = (1, 2, 3)

    def at_xy(a, b, d):
        core = 1 - c if d else c
        return {"dp": zh * 8 + turn(y, b) * 2 + core, "seq": turn(x, a) * 4 + zl}


    def around(o):
        return lax.rem(zh * 4 + zl + o, 16)

    def at_z(o):
        z = around(o)
        return {"dp": lax.div(z, 4) * 8 + y * 2 + c, "seq": x * 4 + lax.rem(z, 4)}
    for peer in peers:
        pl.semaphore_signal(
            barrier, inc=1, device_id=peer, device_id_type=pl.DeviceIdType.MESH
        )
    copies = Copies(send_sem, recv_sem)
    copies.someone = other

    pulls = []

    def pull(src, dst):
        pulls.append(pltpu.make_async_copy(src, dst, own_sem.at[len(pulls)]))
        pulls[-1].start()
        return pulls[-1]

    wt_pull = pull(wt_in, wf.at[:, 0, c])
    qkv_pulls = [pull(value_in, value)]
    for h in range(HEADS):
        cols = pl.ds(h * QK, QK)
        qkv_pulls.append(pull(query_in.at[:, cols], qkv.at[h, :, pl.ds(0, QK)]))
        qkv_pulls.append(pull(key_in.at[:, cols], qkv.at[h, :, pl.ds(QK, QK)]))
    feats_pulls = [pull(gain_in, gain), pull(feats_in, fext.at[pl.ds(RIM, ROWS)])]
    rest_pulls = [
        pull(targets_in, targets),
        pull(offsets_in, offsets),
        pull(mask_in, track_mask),
        pull(pairing_in, pairing),
    ]
    rows = C + HEADS * VD
    head_copies = [pull(head_in, head.at[pl.ds(0, rows)])]
    for a in range(4):
        for b in range(4):
            start = pl.multiple_of(256 * turn(zh, b) + 64 * a, 64)
            block = head_in.at[pl.ds(start, 64)]
            head_copies.append(pull(block, headp.at[a, pl.ds(64 * b, 64)]))
    fext[0:8, :] = jnp.zeros((8, C), bf16)
    fext[2 * RIM + ROWS - 8 :, :] = jnp.zeros((8, C), bf16)
    head[rows:, :] = jnp.zeros((VP - VD, TRACKS), bf16)

    def columns(o, half):
        if half is None:
            return pl.ds(pl.multiple_of(turn(x, o) * 256, 128), 256)
        return pl.ds(pl.multiple_of(turn(x, o) * 256 + 128 * half, 128), 128)

    def slot(t, r, half):
        if half is None:
            return wf.at[t, r, c, :, :, columns(0, None)]
        return wf.at[t, r, c, half, :, columns(0, None)]

    def unit_yx(t, r):
        return lambda o, half: wf.at[t, r, c, :, :, columns(o, half)]

    def unit_of(buf):
        def unit(o, half):
            if half is None:
                return buf.at[turn(y, o)]
            return buf.at[turn(y, o), pl.ds(half * 48, 48), :]

        return unit

    kv_cols = pl.ds(QK, 3 * QK)

    def unit_kv(o, half):
        if half is None:
            return kva.at[turn(x, o), :, :, kv_cols]
        return kva.at[turn(x, o), pl.ds(2 * half, 2), :, kv_cols]

    g_yx = [[Direct(copies, at_x, unit_yx(t, r)) for r in range(4)] for t in range(KW)]
    g_taps = Gather(copies, at_y, unit_of(taps))
    g_weigh = Gather(copies, at_y, unit_of(weigh))
    g_kv = Direct(copies, at_x, unit_kv)
    wt_pull.wait()
    pl.semaphore_wait(barrier, len(peers))
    for pulled in feats_pulls:
        pulled.wait()
    edge = pl.ds(RIM + ROWS, 8)
    lo = copies.start(fext.at[pl.ds(ROWS + 8, 8)], fext.at[pl.ds(8, 8)], after)
    hi = copies.start(fext.at[pl.ds(RIM, 8)], fext.at[edge], before)
    z_in = []
    for t in range(KW):
        right = copies.start(slot(t, 0, None), slot(t, 3, None), at_zh(1))
        left = copies.start(slot(t, 0, None), slot(t, 1, None), at_zh(3))
        z_in.append((right, left))
    pair_in = []

    def share(r, t=None):
        taps_of = pl.ds(0, KW) if t is None else t
        part = wf.at[taps_of, r, c]
        n = copies.start(part, part, other)
        pair_in.append((r, n, wf.at[taps_of, r, 1 - c]))

    share(0)

    for pulled in qkv_pulls:
        pulled.wait()
    lane = iota((TOK, VP), 1)
    vals = value[...].astype(f32)
    for h in range(HEADS):
        start = h * VD
        if h % 2 == 0:
            cut = vals[:, start : start + VP]
        else:
            cut = pltpu.roll(vals[:, start - 64 : start + VD], VP - 64, 1)
        qkv[h, :, 2 * QK :] = jnp.where(lane < VD, cut, 0.0).astype(bf16)
    kva[x, zl] = qkv[zl]
    qkv_in = [
        copies.start(qkv.at[turn(zl, o)], kva.at[x, zl], at_zl(o)) for o in offs
    ]
    def normed(row):
        f = fext[pl.ds(row, 16), :].astype(f32)
        r = lax.rsqrt(jnp.mean(f * f, axis=1, keepdims=True) + NORM_EPS)
        n = f * r
        g = n * gain[...]
        sq = g * g
        t = jnp.tanh(ROOT * (g + CUBIC * (sq * g)))
        return n, g, sq, t, r

    def hidden(row):
        n, g, sq, t, r = normed(row)
        hext[pl.ds(row, 16), :] = (0.5 * g * (1.0 + t)).astype(bf16)

    def slopes(row):
        n, g, sq, t, r = normed(row)
        slope = 0.5 * (1.0 + t) + (0.5 * ROOT) * g * (1.0 - t * t) * (
            1.0 + (3.0 * CUBIC) * sq
        )
        dn = slope * n
        top = dn.astype(bf16)
        dnh[pl.ds(row, 16), :] = top
        dnl[pl.ds(row, 16), :] = (dn - top.astype(f32)).astype(bf16)
        return n, slope, r

    @pl.loop(1, 1 + ROWS // 16)
    def _(i):
        hidden(pl.multiple_of(i * 16, 16))

    for pulled in rest_pulls:
        pulled.wait()
    flip = dp >= PAIRS
    interval = lax.rem(dp, PAIRS)
    sign = jnp.where(flip, -1, 1)
    mine = iota((1, PAIRS), 1) == interval
    chosen = jnp.sum(jnp.where(mine, offsets[...].astype(f32), 0.0), axis=1, keepdims=True)
    off = chosen.astype(jnp.int32) * sign

    EXT = ROWS + 2 * RIM

    def mean_matrix(count, shift_of):
        row, col = iota((count, EXT), 0), iota((count, EXT), 1)
        tok = lax.rem(row, TOK)
        at = col - RIM
        rel = at + off - shift_of(row) - POOL * tok
        where_p = s * ROWS + at + off
        where_q = s * ROWS + at
        fine = (rel >= 0) & (rel < POOL) & (where_p >= 0) & (where_p < L16)
        fine = fine & (where_q >= 0) & (where_q < L16)
        return jnp.where(fine, 1.0 / POOL, 0.0).astype(bf16)

    mix = mean_matrix(KW * TOK, lambda row: (lax.div(row, TOK) - 1) * sign)
    still = mean_matrix(TOK, lambda row: 0 * row)
    copies.arrived(lo, fext.at[pl.ds(8, 8)])
    copies.arrived(hi, fext.at[edge])
    hidden(0)
    hidden(RIM + ROWS)
    taps[y] = dot(mix, hext[...], NN).astype(bf16)
    g_taps.begin()
    pooled_u = dot(still, fext[...], NN).astype(bf16)

    def later(first, last):
        @pl.loop(first, last)
        def _(i):
            row = pl.multiple_of(i * 16, 16)
            n, slope, r = slopes(pl.multiple_of(row + RIM, 16))
            nbuf[pl.ds(row, 16), :] = n
            dbuf[pl.ds(row, 16), :] = slope * gain[...]
            rbuf[pl.ds(row, 16), :] = jnp.broadcast_to(r, (16, 128))

    z_far = []
    for t in range(KW):
        right, left = z_in[t]
        copies.arrived(right, slot(t, 3, None))
        to_right = copies.start(slot(t, 3, 0), slot(t, 2, 0), at_zh(1))
        g_yx[t][3].begin()
        copies.arrived(left, slot(t, 1, None))
        to_left = copies.start(slot(t, 1, 1), slot(t, 2, 1), at_zh(3))
        g_yx[t][1].begin()
        z_far.append((to_right, to_left))
    for o, n in zip(offs, qkv_in):
        copies.arrived(n, kva.at[x, turn(zl, 4 - o)])
    g_kv.begin()
    g_taps.relay()
    for pulled in head_copies:
        pulled.wait()
    pre[...] = dot(pooled_u, head[0:C, :], NN)
    def spread(width, tap_of):
        row, col = iota((ROWS, width), 0), iota((ROWS, width), 1)
        reach = row + off - tap_of(col)
        at = s * ROWS + row + off
        seen = s * ROWS + reach
        fine = (lax.shift_right_arithmetic(reach + 64, 3) == lax.rem(col, 64)) & (at >= 0)
        fine = fine & (at < L16) & (seen >= 0) & (seen < L16)
        return jnp.where(fine, 1.0, 0.0).astype(bf16)

    three[...] = spread(192, lambda col: (lax.div(col, 64) - 1) * sign)
    one[...] = spread(64, lambda col: 0 * col)
    dyt[...] = jnp.zeros((64, C), f32)
    zall[...] = jnp.zeros((KW, 64, C), f32)
    edges[...] = jnp.zeros((16, 256), f32)
    zr_f[...] = jnp.zeros((4, 8, C), f32)

    later(0, 8)
    for t in range(KW):
        to_right, to_left = z_far[t]
        copies.arrived(to_right, slot(t, 2, 0))
        copies.arrived(to_left, slot(t, 2, 1))
        g_yx[t][2].begin()
    for r in (3, 1):
        for t in range(KW):
            g_yx[t][r].end()
        share(r)
    g_taps.end()

    def convolve(r):
        for q, n, part in pair_in:
            if q == r:
                copies.arrived(n, part)
        acc = jnp.zeros((4 * TOK, 64), f32)
        for t in range(KW):
            rows_t = taps[:, t * TOK : (t + 1) * TOK, :].reshape(4 * TOK, C)
            acc = acc + dot(rows_t, wf[t, r].reshape(64, C), NT)
        cv_s[:, :, r * 64 : (r + 1) * 64] = acc.astype(bf16).reshape(4, TOK, 64)

    convolve(0)
    for t in range(KW):
        g_yx[t][2].end()
        share(2, t)
    g_kv.end()
    inv_sqrt = 1.0 / math.sqrt(QK)
    qh = kva[x, :, :, 0:QK].reshape(4 * TOK, QK)
    kh = kva[:, :, :, QK : 2 * QK].reshape(16 * TOK, QK)
    vh = kva[:, :, :, 2 * QK :].reshape(16 * TOK, VP)
    scores = dot(qh, kh, NT) * inv_sqrt
    e = jnp.exp(scores - jnp.max(scores, axis=1, keepdims=True))
    p = e / jnp.sum(e, axis=1, keepdims=True)
    probs[...] = p
    probs_b[...] = p.astype(bf16)
    att_s[...] = dot(probs_b[...], vh, NN).astype(bf16).reshape(4, TOK, VP)
    att_r[zl] = att_s[zl]
    att_in = [
        copies.start(att_s.at[turn(zl, o)], att_r.at[zl], at_zl(o)) for o in offs
    ]
    convolve(3)
    convolve(1)
    convolve(2)
    cv_r[y] = cv_s[y]
    cv_in = [copies.start(cv_s.at[turn(y, o)], cv_r.at[y], at_y(o)) for o in offs]
    tgt_s[...] = targets[...].astype(bf16)
    tgt_in = copies.start(tgt_s, tgt_r, at_zh(2))
    slopes(0)
    slopes(RIM + ROWS)
    later(8, 16)
    both = dot(mix, dnh[...], NN) + dot(mix, dnl[...], NN)
    weigh[y] = (both * POOL).astype(bf16)
    g_weigh.begin()
    pick[...] = jnp.where(
        iota((TRACKS, TRACKS), 0) == pairing[...], 1.0, 0.0
    ).astype(bf16)
    mrow = track_mask[pl.ds(interval, 1), :].astype(f32)
    count = jnp.maximum(jnp.sum(mrow, axis=1, keepdims=True), 1.0)
    mpair = dot(jnp.broadcast_to(mrow, (16, TRACKS)).astype(bf16), pick[...], NN)[0:1, :]
    for o, n in zip(offs, att_in):
        copies.arrived(n, att_r.at[turn(zl, 4 - o)])
    for h in range(HEADS):
        pre[...] += dot(att_r[h], head[C + h * VD : C + h * VD + VP, :], NN)
    for o, n in zip(offs, cv_in):
        copies.arrived(n, cv_r.at[turn(y, 4 - o)])

    logits = pre[...]
    for a in range(4):
        logits = logits + dot(cv_r[a], headp[a], NN)
    pred = jnp.maximum(logits, 0.0) + jnp.log1p(jnp.exp(-jnp.abs(logits)))
    pred_s[...] = pred.astype(bf16)
    pred_in = copies.start(pred_s, pred_r, at_zh(2))
    gate = jax.nn.sigmoid(logits)
    copies.arrived(tgt_in, tgt_r)
    tgt_p[...] = dot(tgt_r[...], pick[...], NN)
    g_weigh.relay()
    copies.arrived(pred_in, pred_r)
    both = 0.5 * (pred + dot(pred_r[...], pick[...], NN))
    misfit = both - targets[...]
    weighted = mrow * misfit
    dpred = (LOSS_SCALE / count) * (weighted + mpair * (both - tgt_p[...]))
    dlogit = (dpred * gate).astype(bf16)

    for a in range(4):
        part = dot(dlogit, headp[a], NT) * (1.0 / POOL)
        dyp_s[a] = part.astype(bf16)
    dyp_r[y] = dyp_s[y]
    dyp_in = [copies.start(dyp_s.at[turn(y, o)], dyp_r.at[y], at_y(o)) for o in offs]
    for h in range(HEADS):
        part = dot(dlogit, head[C + h * VD : C + h * VD + VP, :], NT)
        datt_s[h] = jnp.where(lane < VD, part, 0.0).astype(bf16)
    datt_r[zl] = datt_s[zl]
    datt_in = [
        copies.start(datt_s.at[turn(zl, o)], datt_r.at[zl], at_zl(o)) for o in offs
    ]
    dyt[8 : 8 + TOK, :] = dot(dlogit, head[0:C, :], NT) * (1.0 / POOL)
    rim_s[0] = dyt[8:9, :]
    rim_s[1] = dyt[7 + TOK : 8 + TOK, :]
    rim_hi = copies.start(rim_s.at[0], rim_r.at[0], before)
    rim_lo = copies.start(rim_s.at[1], rim_r.at[1], after)

    loss = jnp.sum(jnp.sum(weighted * misfit, axis=1, keepdims=True), axis=0, keepdims=True)
    loss = loss / count / (2.0 * PAIRS * TOK * 16)
    g_weigh.end()
    for o, n in zip(offs, dyp_in):
        copies.arrived(n, dyp_r.at[turn(y, 4 - o)])
    for a in range(4):
        cols = slice(a * 256, (a + 1) * 256)
        edge_s[0, :, cols] = dyp_r[a, 0:1, :].astype(f32)
        edge_s[1, :, cols] = dyp_r[a, TOK - 1 : TOK, :].astype(f32)
    edge_hi = copies.start(edge_s.at[0], edge_r.at[0], before)
    edge_lo = copies.start(edge_s.at[1], edge_r.at[1], after)
    @pl.loop(0, 4)
    def _(b):
        cols = pl.ds(pl.multiple_of(b * 256, 256), 256)
        gains = jnp.zeros((4 * TOK, 256), f32)
        dyr = dyp_r[...].reshape(4 * TOK, 256)
        for t in range(KW):
            part = pl.ds(t * TOK, TOK)
            w = wf[t, :, :, :, :, cols].reshape(256, 256)
            acc = dot(dyr, w, NN)
            zp_s[:, part, cols] = acc.astype(bf16).reshape(4, TOK, 256)
            gains = gains + acc * weigh[:, part, cols].reshape(4 * TOK, 256).astype(f32)
        gacc[:, cols] = jnp.sum(gains, axis=0, keepdims=True)

    zp_in = [copies.start(zp_s.at[turn(y, o)], zp_r.at[y], at_y(o)) for o in offs]
    zp_r[y] = zp_s[y]

    ar_z[around(0)] = jnp.concatenate(
        [gacc[...], jnp.broadcast_to(loss, (1, 128))], axis=1
    )
    ring = (8, 7, 9, 6, 10, 5, 11, 4, 12, 3, 13, 2, 14, 1, 15)
    ar_in = [copies.start(ar_z.at[around(0)], ar_z.at[around(0)], at_z(o)) for o in ring]
    for o, n in zip(offs, datt_in):
        copies.arrived(n, datt_r.at[turn(zl, 4 - o)])
    dout = datt_r[...].reshape(4 * TOK, VP)
    att = att_s[...].reshape(4 * TOK, VP)
    delta = jnp.sum(dout.astype(f32) * att.astype(f32), axis=1, keepdims=True)
    vh = kva[:, :, :, 2 * QK :].reshape(16 * TOK, VP)
    ds = (probs[...] * (dot(dout, vh, NT) - delta)).astype(bf16)
    qh = kva[x, :, :, 0:QK].reshape(4 * TOK, QK)
    kvp_s[:, :, :, 0:QK] = dot(ds, qh, TN).astype(bf16).reshape(4, 4, TOK, QK)
    kvp_s[:, :, :, QK:] = dot(probs_b[...], dout, TN).astype(bf16).reshape(4, 4, TOK, VP)
    kvp_in = [copies.start(kvp_s.at[turn(x, o)], kvp_r.at[x], at_x(o)) for o in offs]
    kh = kva[:, :, :, QK : 2 * QK].reshape(16 * TOK, QK)
    dq_s[...] = (dot(ds, kh, NN) * inv_sqrt).astype(bf16).reshape(4, TOK, QK)
    dq_r[zl] = dq_s[zl]
    dq_in = [copies.start(dq_s.at[turn(zl, o)], dq_r.at[zl], at_zl(o)) for o in offs]
    copies.arrived(edge_hi, edge_r.at[0])
    copies.arrived(edge_lo, edge_r.at[1])
    for a in range(4):
        cols = slice(a * 256, (a + 1) * 256)
        edges[a : a + 1, :] = edge_r[0][:, cols]
        edges[8 + a : 9 + a, :] = edge_r[1][:, cols]
    both = edges[...].astype(bf16)
    for t in range(KW):
        res = dot(both, wf[t].reshape(256, C), NN)
        for a in range(4):
            zr_f[a, t : t + 1, :] = res[a : a + 1, :]
            zr_f[a, KW + t : KW + t + 1, :] = res[8 + a : 9 + a, :]
    zr_s[...] = zr_f[...].astype(bf16)
    zr_r[y] = zr_s[y]
    zr_in = [copies.start(zr_s.at[turn(y, o)], zr_r.at[y], at_y(o)) for o in offs]
    for o, n in zip(offs, kvp_in):
        copies.arrived(n, kvp_r.at[turn(x, 4 - o)])
    total = kvp_s[x].astype(f32)
    for o in offs:
        total = total + kvp_r[turn(x, o)].astype(f32)
    kvg_s[:, :, 0:QK] = (total[:, :, 0:QK] * inv_sqrt).astype(bf16)
    kvg_s[:, :, QK:] = total[:, :, QK:].astype(bf16)
    kvg_r[zl] = kvg_s[zl]
    kvg_in = [
        copies.start(kvg_s.at[turn(zl, o)], kvg_r.at[zl], at_zl(o)) for o in offs
    ]
    for o, n in zip(ring, ar_in):
        copies.arrived(n, ar_z.at[around(16 - o)])
    total = jnp.zeros((1, ROW), f32)
    for a in range(0, 16, 4):
        total = total + ((ar_z[a] + ar_z[a + 1]) + (ar_z[a + 2] + ar_z[a + 3]))
    ar_p[x, y, c] = total
    plane = [(a, b, d) for a in (2, 1, 3, 0) for b in (2, 1, 3, 0) for d in (0, 1) if a or b or d]
    mine_p = ar_p.at[x, y, c]
    ar_in = [copies.start(mine_p, mine_p, at_xy(a, b, d)) for a, b, d in plane]
    for o, n in zip(offs, zp_in):
        copies.arrived(n, zp_r.at[turn(y, 4 - o)])

    @pl.loop(0, 4)
    def _(b):
        cols = pl.ds(pl.multiple_of(b * 256, 256), 256)
        for t in range(KW):
            part = pl.ds(t * TOK, TOK)
            low = zp_r[0, part, cols].astype(f32) + zp_r[1, part, cols].astype(f32)
            high = zp_r[2, part, cols].astype(f32) + zp_r[3, part, cols].astype(f32)
            zall[t, 8 : 8 + TOK, cols] = low + high

    copies.arrived(rim_hi, rim_r.at[0])
    copies.arrived(rim_lo, rim_r.at[1])
    for o, n in zip(offs, zr_in):
        copies.arrived(n, zr_r.at[turn(y, 4 - o)])
    low = zr_r[0].astype(f32) + zr_r[1].astype(f32)
    beside = low + (zr_r[2].astype(f32) + zr_r[3].astype(f32))
    for t in range(KW):
        zall[t, 8 + TOK : 9 + TOK, :] = beside[t : t + 1, :]
        zall[t, 7:8, :] = beside[KW + t : KW + t + 1, :]
    dyt[7:8, :] = rim_r[1]
    dyt[8 + TOK : 9 + TOK, :] = rim_r[0]

    @pl.loop(0, 4)
    def _(b):
        cols = pl.ds(pl.multiple_of(b * 256, 256), 256)

        def exact(mat, val):
            top = val.astype(bf16)
            low = (val - top.astype(f32)).astype(bf16)
            return dot(mat, top, NN) + dot(mat, low, NN)

        dhb[:, cols] = exact(three[...], zall[:, :, cols].reshape(KW * 64, 256))
        dyb[:, cols] = exact(one[...], dyt[:, cols])

    @pl.loop(0, ROWS // 16)
    def _(i):
        at = pl.ds(pl.multiple_of(i * 16, 16), 16)
        n = nbuf[at, :]
        dn = dhb[at, :] * dbuf[at, :]
        mid = jnp.mean(dn * n, axis=1, keepdims=True)
        r = rbuf[at, :][:, 0:1]
        dfeats[at, :] = (r * (dn - n * mid) + dyb[at, :]).astype(bf16)

    for o, n in zip(offs, dq_in):
        copies.arrived(n, dq_r.at[turn(zl, 4 - o)])
    for h in range(HEADS):
        dquery[:, h * QK : (h + 1) * QK] = dq_r[h]
    for o, n in zip(offs, kvg_in):
        copies.arrived(n, kvg_r.at[turn(zl, 4 - o)])
    for h in range(HEADS):
        dkey[:, h * QK : (h + 1) * QK] = kvg_r[h, :, 0:QK]
    for h in (0, 2):
        even = kvg_r[h, :, QK:].astype(f32)
        odd = pltpu.roll(kvg_r[h + 1, :, QK:].astype(f32), VD, 1)
        start = h * VD
        dvalue[:, start : start + VP] = jnp.where(lane < VD, even, odd).astype(bf16)
        dvalue[:, start + VP : start + VP + 128] = odd[:, 0:128].astype(bf16)

    for (a, b, d), n in zip(plane, ar_in):
        from_core = 1 - c if d else c
        copies.arrived(n, ar_p.at[turn(x, 4 - a), turn(y, 4 - b), from_core])
    total = jnp.zeros((1, ROW), f32)
    for a in range(4):
        for b in range(4):
            total = total + (ar_p[a, b, 0] + ar_p[a, b, 1])
    dgain[...] = total[:, 0:C]
    loss_out[...] = total[:, C:]
    copies.finish()


def store_kernel(*refs):
    sems = refs[12]
    puts = [pltpu.make_async_copy(refs[i], refs[6 + i], sems.at[i]) for i in range(6)]
    for put in puts:
        put.start()
    for put in puts:
        put.wait()


def body(
    features,
    shift_offsets,
    conv_weight,
    norm_gain,
    query_proj,
    key_proj,
    value_proj,
    head_weight,
    targets,
    track_mask,
    track_pairing,
):
    wt = jnp.swapaxes(conv_weight, 1, 2).reshape(KW, 2, 16, C)
    vmem = pl.BlockSpec(memory_space=pltpu.VMEM)
    hbm = pl.BlockSpec(memory_space=pltpu.HBM)
    V = pltpu.VMEM
    scratch = [
        V((1, PAIRS), jnp.int32),
        V((1, C), f32),
        V((TOK, HEADS * VD), bf16),
        V((TOK, TRACKS), f32),
        V((PAIRS, TRACKS), jnp.int32),
        V((1, TRACKS), jnp.int32),
        V((KW, 4, 2, 2, 16, C), bf16),
        V((ROWS + 2 * RIM, C), bf16),
        V((ROWS + 2 * RIM, C), bf16),
        V((ROWS + 2 * RIM, C), bf16),
        V((ROWS + 2 * RIM, C), bf16),
        V((ROWS, C), f32),
        V((ROWS, C), f32),
        V((ROWS, 128), f32),
        V((C + HEADS * VD + VP - VD, TRACKS), bf16),
        V((4, 256, TRACKS), bf16),
        V((4, TOK, 512), bf16),
        V((4, 4, TOK, 512), bf16),
        V((4, TOK, VP), bf16),
        V((4, TOK, VP), bf16),
        V((4 * TOK, 16 * TOK), f32),
        V((4 * TOK, 16 * TOK), bf16),
        V((4, KW * TOK, C), bf16),
        V((4, KW * TOK, C), bf16),
        V((4, TOK, 256), bf16),
        V((4, TOK, 256), bf16),
        V((4, TOK, 256), bf16),
        V((4, TOK, 256), bf16),
        V((4, KW * TOK, C), bf16),
        V((4, KW * TOK, C), bf16),
        V((TOK, TRACKS), f32),
        V((TOK, TRACKS), bf16),
        V((TOK, TRACKS), bf16),
        V((TOK, TRACKS), bf16),
        V((TOK, TRACKS), bf16),
        V((TRACKS, TRACKS), bf16),
        V((TOK, TRACKS), f32),
        V((ROWS, KW * 64), bf16),
        V((ROWS, 64), bf16),
        V((4, TOK, VP), bf16),
        V((4, TOK, VP), bf16),
        V((4, TOK, QK), bf16),
        V((4, TOK, QK), bf16),
        V((4, 4, TOK, 384), bf16),
        V((4, 4, TOK, 384), bf16),
        V((4, TOK, 384), bf16),
        V((4, TOK, 384), bf16),
        V((64, C), f32),
        V((KW, 64, C), f32),
        V((2, 1, C), f32),
        V((2, 1, C), f32),
        V((2, 1, C), f32),
        V((2, 1, C), f32),
        V((16, 256), f32),
        V((4, 8, C), f32),
        V((4, 8, C), bf16),
        V((4, 8, C), bf16),
        V((ROWS, C), f32),
        V((ROWS, C), f32),
        V((1, C), f32),
        V((4, 4, 2, 1, ROW), f32),
        V((16, 1, ROW), f32),
        pltpu.SemaphoreType.DMA((COPIES,)),
        pltpu.SemaphoreType.DMA((COPIES,)),
        pltpu.SemaphoreType.DMA((36,)),
    ]
    out = jax.ShapeDtypeStruct
    outs = pl.pallas_call(
        step_kernel,
        name="strand_step",
        out_shape=(
            out((ROWS, C), bf16),
            out((TOK, HEADS * QK), bf16),
            out((TOK, HEADS * QK), bf16),
            out((TOK, HEADS * VD), bf16),
            out((1, C), f32),
            out((1, 128), f32),
        ),
        in_specs=[hbm] * 11,
        out_specs=(vmem,) * 6,
        scratch_shapes=scratch,
        compiler_params=pltpu.CompilerParams(
            collective_id=0, has_side_effects=True, vmem_limit_bytes=48 << 20
        ),
    )(
        *(
            pltpu.with_memory_space_constraint(a, pltpu.HBM)
            for a in (
                features[0],
                shift_offsets.reshape(1, PAIRS),
                wt,
                norm_gain.reshape(1, C),
                query_proj[0],
                key_proj[0],
                value_proj[0],
                head_weight,
                targets[0],
                track_mask,
                track_pairing.reshape(1, TRACKS),
            )
        )
    )
    outs = pl.pallas_call(
        store_kernel,
        name="store",
        out_shape=tuple(out(o.shape, o.dtype) for o in outs),
        in_specs=[vmem] * 6,
        out_specs=(hbm,) * 6,
        scratch_shapes=[pltpu.SemaphoreType.DMA((6,))],
        compiler_params=pltpu.CompilerParams(vmem_limit_bytes=4 << 20),
    )(*outs)
    features_grad, query_grad, key_grad, value_grad, gain_grad, loss = outs
    return (
        features_grad[None],
        query_grad[None],
        key_grad[None],
        value_grad[None],
        gain_grad.reshape(C),
        loss[0, 0],
    )


def solution(mesh):
    placed = (
        P("dp", "seq", None),
        P(),
        P(None, None, "dp"),
        P(),
        P("dp", "seq", None),
        P("dp", "seq", None),
        P("dp", "seq", None),
        P(),
        P("dp", "seq", None),
        P(),
        P(),
    )
    return jax.shard_map(
        body,
        mesh=mesh,
        in_specs=placed,
        out_specs=(
            P("dp", "seq", None),
            P("dp", "seq", None),
            P("dp", "seq", None),
            P("dp", "seq", None),
            P(),
            P(),
        ),
        check_vma=False,
    )
```
